256 devices in a mesh: member: 8 (over z_hi, core), space: 16 (over x, y), group: 2 (over z_lo).
Axes of the slice: x: 4, y: 4, z: 8 (z_hi: 4, z_lo: 2; z = z_hi * 2 + z_lo), core: 2. Of those that a mesh axis runs over, the one named last changes fastest.
Arguments:
- ensemble: bfloat16 [2, 512, 3, 64, 512], P('group', 'member', None, 'space'), may hold values from -6 to 6
- obs_index: int32 [2, 16, 8, 256], P('group', 'space'), may hold values from 0 to 255
- obs_value: float32 [2, 16, 8, 256], P('group', 'space', 'member'), may hold values from -6 to 6
- obs_var: float32 [2, 16, 8, 256], P('group', 'space', 'member'), may hold values from 0.3 to 3
Outputs:
- analysis: bfloat16 [2, 512, 3, 64, 512], P('group', 'member', None, 'space')
The draws below stay inside these ranges and needn't reach their ends.
Inputs may be any that keep to these rules, and one draw needn't show every extreme that they name: `obs_index`: each entry names a cell of its region's tile, counted row by row over 64 columns; cells may repeat.
All inputs are finite; a program needn't handle non-finite values.
Results may differ from the reference program's by a relative error of at most 0.0075.
Values may be sent and summed in bfloat16 or wider, within the bound.
No kernel may reach another device: no remote copies, remote signals or barrier semaphores. Data moves between devices by JAX's collectives and lax.ppermute only.
A program may use at most 64 MiB of HBM per device.

```python
import math
import jax
import jax.numpy as jnp
from jax import lax

MEMBERS = 512
MESH_WIDTH = 512
ROWS_DEV = 4
OBS = 256
STEPS = 2
NS_STEPS = 6
MESH_LATITUDES = 64
PATCH_DOWNWARD = 16
PATCH_ACROSS = 8
CELLS = 256
N_MEMBER = 8
N_GROUP = 2


def plant(drawn, rng, low, largest):
    spot = [jax.random.randint(jax.random.fold_in(rng, axis), (), 0, length) for axis, length in enumerate(drawn.shape)]
    main_axis = drawn.shape.index(max(drawn.shape))
    neighbour = spot[:main_axis] + [(spot[main_axis] + 1) % drawn.shape[main_axis]] + spot[main_axis + 1:]
    return drawn.at[tuple(spot)].set(low).at[tuple(neighbour)].set(largest)


def block_scale(key, dims, cuts, least, top_value):
    def one(position, blocks):
        draws = jax.random.uniform(jax.random.fold_in(jax.random.fold_in(key, 6), position), (blocks,), jnp.float32, least / len(cuts), top_value / len(cuts))
        return jnp.repeat(jnp.exp(draws), dims[position] // blocks).reshape((-1,) + (1,) * (len(dims) - position - 1))

    gain = one(*cuts[0])
    for cut in cuts[1:]:
        gain = gain * one(*cut)
    return gain


def centred(stream_key, shape, width, bound, cuts=(), kind=jnp.bfloat16):
    array = jax.random.normal(stream_key, shape, jnp.float32) * width
    if len(cuts) > 0:
        array = block_scale(stream_key, shape, cuts, -0.22, 0.18) * array
    return jnp.clip(array, min=-bound, max=bound).astype(kind)


def setup_inputs(seed: int = 0) -> dict:
    key_list = jax.random.split(jax.random.key(seed), 5)
    return {
        "ensemble": centred(key_list[0], (N_GROUP, MEMBERS, 3, MESH_LATITUDES, MESH_WIDTH), 1.0, 6.0, ((0, 2), (1, 8), (3, 16))),
        "obs_index": plant(jax.random.randint(key_list[1], (N_GROUP, PATCH_DOWNWARD, PATCH_ACROSS, OBS), 0, CELLS), jax.random.fold_in(key_list[1], 1), 0, CELLS - 1).astype(jnp.int32),
        "obs_value": centred(key_list[2], (N_GROUP, PATCH_DOWNWARD, PATCH_ACROSS, OBS), 1.0, 6.0, ((0, 2), (1, 16), (2, 8)), jnp.float32),
        "obs_var": jnp.clip(jnp.exp(math.log(3.0) - 2.3025851 * jax.random.uniform(key_list[3], (N_GROUP, PATCH_DOWNWARD, PATCH_ACROSS, OBS), jnp.float32) ** block_scale(key_list[3], (N_GROUP, PATCH_DOWNWARD, PATCH_ACROSS, OBS), ((0, 2), (1, 16), (2, 8)), -0.2, 0.2)), 0.3, 3.0),
    }


time_step = 0.4
coriolis = 0.3

def tendency(height, northward, eastward):
    d_height = -(0.5 * (jnp.roll(eastward, -1, -1) - jnp.roll(eastward, 1, -1)) + 0.5 * (northward[..., 2:, :] - northward[..., :-2, :]))
    d_north = -0.5 * (height[..., 2:, :] - height[..., :-2, :]) - coriolis * eastward
    d_east = -0.5 * (jnp.roll(height, -1, -1) - jnp.roll(height, 1, -1))[..., 1:-1, :] + coriolis * northward[..., 1:-1, :]
    return jnp.stack((d_height, d_north, d_east), axis=1)

def wrap_rows(section):
    return jnp.concatenate((section[..., -1:, :], section, section[..., :1, :]), axis=-2)

def segment_rates(present_states):
    padded = wrap_rows(present_states[:, 0:2])
    return tendency(padded[:, 0], padded[:, 1], present_states[:, 2])

def predicted_patch_slab(patch_slab):
    present_states = patch_slab.astype(jnp.float32)
    for repeat in range(STEPS):
        segment_one = present_states + time_step * segment_rates(present_states)
        segment_two = 0.75 * present_states + 0.25 * (segment_one + time_step * segment_rates(segment_one))
        present_states = present_states / 3.0 + 2.0 / 3.0 * (segment_two + time_step * segment_rates(segment_two))
    return present_states.astype(jnp.bfloat16)

def region_weights(sampled, values, variances):
    sample_states = sampled.shape[0]
    high = lax.Precision.HIGHEST
    mean_obs = lax.optimization_barrier(jnp.mean(sampled, axis=0))
    spread = sampled - mean_obs
    scaled = spread / variances
    identity = jnp.eye(sample_states, dtype=jnp.float32)
    gram = (sample_states - 1.0) * identity + jnp.dot(scaled, spread.T, precision=high, preferred_element_type=jnp.float32)
    drive = jnp.dot(scaled, values - mean_obs, precision=high, preferred_element_type=jnp.float32)
    norm_f = jnp.sqrt(jnp.sum(gram * gram))
    upper_part = gram / norm_f
    lower_part = identity
    for repeat in range(NS_STEPS):
        step_matrix = 1.5 * identity - 0.5 * jnp.dot(lower_part, upper_part, precision=high, preferred_element_type=jnp.float32)
        upper_part = jnp.dot(upper_part, step_matrix, precision=high, preferred_element_type=jnp.float32)
        lower_part = jnp.dot(step_matrix, lower_part, precision=high, preferred_element_type=jnp.float32)
    root = lower_part / jnp.sqrt(norm_f)
    centre = jnp.dot(root, jnp.dot(root, drive, precision=high, preferred_element_type=jnp.float32), precision=high, preferred_element_type=jnp.float32)
    return (math.sqrt(sample_states - 1.0) * root + centre[:, None]).astype(jnp.bfloat16)

def blend(deviation, tile_mean, corner):
    sample_states, fields, latitude_number, longitude_number = deviation.shape
    half_rows = latitude_number // 2
    half_cols = longitude_number // 2
    row_weight = jnp.abs((jnp.arange(latitude_number, dtype=jnp.float32) + 0.5) / latitude_number - 0.5)
    col_weight = jnp.abs((jnp.arange(longitude_number, dtype=jnp.float32) + 0.5) / longitude_number - 0.5)
    bands = []
    for row_half in range(2):
        pieces = []
        row_part = slice(row_half * half_rows, (row_half + 1) * half_rows)
        row_step = -1 if row_half == 0 else 1
        for col_half in range(2):
            col_part = slice(col_half * half_cols, (col_half + 1) * half_cols)
            col_step = -1 if col_half == 0 else 1
            quarter = deviation[:, :, row_part, col_part].reshape(sample_states, -1)
            row_near = row_weight[row_part][:, None]
            col_near = col_weight[col_part][None, :]
            summed = tile_mean[:, row_part, col_part]
            terms = ((1, 1, (1.0 - row_near) * (1.0 - col_near)), (1 + row_step, 1, row_near * (1.0 - col_near)), (1, 1 + col_step, (1.0 - row_near) * col_near), (1 + row_step, 1 + col_step, row_near * col_near))
            for row_pick, col_pick, factor in terms:
                product = lax.dot_general(corner[row_pick, col_pick], quarter, (((0,), (0,)), ((), ())), preferred_element_type=jnp.float32)
                summed = summed + factor * product.reshape(sample_states, fields, half_rows, half_cols)
            pieces.append(summed)
        bands.append(jnp.concatenate(pieces, axis=3))
    return jnp.concatenate(bands, axis=2).astype(jnp.bfloat16)

def reference(ensemble, obs_index, obs_value, obs_var):
    sample_states = MEMBERS
    latitude_number = ROWS_DEV
    longitude_number = MESH_WIDTH // PATCH_ACROSS
    patch_sequence = PATCH_DOWNWARD * PATCH_ACROSS
    outputs = []
    for stream in range(2):
        patch_slabs = ensemble[stream].reshape(N_MEMBER, sample_states // N_MEMBER, 3, MESH_LATITUDES, MESH_WIDTH)
        predicted_states = lax.map(predicted_patch_slab, patch_slabs).reshape(sample_states, 3, MESH_LATITUDES, MESH_WIDTH)
        subdomain_parts = predicted_states.reshape(sample_states, 3, PATCH_DOWNWARD, latitude_number, PATCH_ACROSS, longitude_number).transpose(2, 4, 0, 1, 3, 5).reshape(patch_sequence, sample_states, 3, latitude_number, longitude_number)

        def one_region(inputs):
            tile, index_row, value_row, var_row = inputs
            sampled = jnp.take(tile[:, 0].reshape(sample_states, -1), index_row, axis=1).astype(jnp.float32)
            return region_weights(sampled, value_row, var_row)
        weights = lax.map(one_region, (subdomain_parts, obs_index[stream].reshape(patch_sequence, OBS), obs_value[stream].reshape(patch_sequence, OBS), obs_var[stream].reshape(patch_sequence, OBS)))
        weights = weights.reshape(PATCH_DOWNWARD, PATCH_ACROSS, sample_states, sample_states)

        def one_blend(inputs):
            tile, place = inputs
            band = place // PATCH_ACROSS
            column = place % PATCH_ACROSS
            row_ids = (band + jnp.arange(-1, 2, dtype=jnp.int32)) % PATCH_DOWNWARD
            col_ids = (column + jnp.arange(-1, 2, dtype=jnp.int32)) % PATCH_ACROSS
            corner = weights[row_ids][:, col_ids]
            tile_mean = lax.optimization_barrier(jnp.mean(tile.astype(jnp.float32), axis=0))
            deviation = (tile.astype(jnp.float32) - tile_mean).astype(jnp.bfloat16)
            return blend(deviation, tile_mean, corner)
        analysed = lax.map(one_blend, (subdomain_parts, jnp.arange(patch_sequence, dtype=jnp.int32)))
        outputs.append(analysed.reshape(PATCH_DOWNWARD, PATCH_ACROSS, sample_states, 3, latitude_number, longitude_number).transpose(2, 3, 0, 4, 1, 5).reshape(sample_states, 3, MESH_LATITUDES, MESH_WIDTH))
    return jnp.stack(outputs)
```

```python
import math

import jax
import jax.numpy as jnp
from jax import lax
from jax.experimental import pallas as pl
from jax.experimental.pallas import tpu as pltpu
from jax.sharding import PartitionSpec as P

STEPS = 2
NS_STEPS = 6
MEMBERS = 512
CELLS = 256
OBS = 256
BLOCK = 128
PAIRS = [(i, j) for i in range(4) for j in range(i, 4)]
CENTRE_AT = len(PAIRS) * BLOCK
PACKED = CENTRE_AT + 4 * 16

time_step = 0.4
coriolis = 0.3
COLS = 768
HALF = 384
f32 = jnp.float32
bf16 = jnp.bfloat16
vmem = pl.BlockSpec(memory_space=pltpu.VMEM)
smem = pl.BlockSpec(memory_space=pltpu.SMEM)


def column_difference(field):
    columns = field.shape[-1]
    return 0.5 * (pltpu.roll(field, columns - 1, 1) - pltpu.roll(field, 1, 1))


def rates(h, v, u, i):
    d_height = -(column_difference(u[i]) + 0.5 * (v[i + 1] - v[i - 1]))
    d_north = -0.5 * (h[i + 1] - h[i - 1]) - coriolis * u[i]
    return d_height, d_north


def rate_east(h, v, i):
    return coriolis * v[i] - column_difference(h[i])


def advance(h0, v0, u0):
    h1, v1, u1, h2, v2, u2, h3, v3, u3 = ({} for _ in range(9))
    for i in range(-2, 6):
        dh, dv = rates(h0, v0, u0, i)
        h1[i] = h0[i] + time_step * dh
        v1[i] = v0[i] + time_step * dv
        if -1 <= i <= 4:
            u1[i] = u0[i] + time_step * rate_east(h0, v0, i)
    for i in range(-1, 5):
        dh, dv = rates(h1, v1, u1, i)
        h2[i] = 0.75 * h0[i] + 0.25 * (h1[i] + time_step * dh)
        v2[i] = 0.75 * v0[i] + 0.25 * (v1[i] + time_step * dv)
        if 0 <= i <= 3:
            u2[i] = 0.75 * u0[i] + 0.25 * (u1[i] + time_step * rate_east(h1, v1, i))
    third = 1.0 / 3.0
    two_thirds = 2.0 / 3.0
    for i in range(4):
        dh, dv = rates(h2, v2, u2, i)
        h3[i] = h0[i] * third + two_thirds * (h2[i] + time_step * dh)
        v3[i] = v0[i] * third + two_thirds * (v2[i] + time_step * dv)
        u3[i] = u0[i] * third + two_thirds * (u2[i] + time_step * rate_east(h2, v2, i))
    return h3, v3, u3


GROUP = 16


def loaded(now, below, above, at):
    h, v, u = {}, {}, {}
    for f, field in enumerate((h, v, u)):
        for i in range(4):
            field[i] = now[f, i, at, :].astype(f32)
    for k in range(3):
        h[k - 3] = below[k, at, :].astype(f32)
        v[k - 3] = below[3 + k, at, :].astype(f32)
        h[4 + k] = above[k, at, :].astype(f32)
        v[4 + k] = above[3 + k, at, :].astype(f32)
    for k in range(2):
        u[k - 2] = below[6 + k, at, :].astype(f32)
        u[4 + k] = above[6 + k, at, :].astype(f32)
    return h, v, u


def first_step_kernel(now, below, above, out, first, last):
    def group(g, carry):
        at = pl.ds(pl.multiple_of(g * GROUP, GROUP), GROUP)
        fields = advance(*loaded(now, below, above, at))
        for f in range(3):
            edge = 2 if f == 2 else 3
            for i in range(4):
                out[f, i, at, :] = fields[f][i]
                if i < edge:
                    first[3 * f + i, at, :] = fields[f][i].astype(bf16)
                if i >= 4 - edge:
                    last[3 * f + i - (4 - edge), at, :] = fields[f][i].astype(bf16)
        return carry

    lax.fori_loop(0, now.shape[2] // GROUP, group, 0)


def last_step_kernel(now, below, above, out):
    lane = lax.broadcasted_iota(jnp.int32, (GROUP, BLOCK), 1) < 64

    def group(g, carry):
        at = pl.ds(pl.multiple_of(g * GROUP, GROUP), GROUP)
        fields = advance(*loaded(now, below, above, at))
        for f in range(3):
            for p in range(2):
                to = p * HALF + f * BLOCK
                for t in range(4):
                    x = fields[f][2 * p][:, t * BLOCK : (t + 1) * BLOCK]
                    y = fields[f][2 * p + 1][:, t * BLOCK : (t + 1) * BLOCK]
                    even = jnp.where(lane, x, pltpu.roll(y, 64, 1))
                    odd = jnp.where(lane, pltpu.roll(x, 64, 1), y)
                    out[2 * t, at, to : to + BLOCK] = even.astype(bf16)
                    out[2 * t + 1, at, to : to + BLOCK] = odd.astype(bf16)
        return carry

    lax.fori_loop(0, now.shape[2] // GROUP, group, 0)


def forecast(fields, up, down):
    _, rows, members, columns = fields.shape
    last = jnp.concatenate([fields[0, 1:], fields[1, 1:], fields[2, 2:]], axis=0)
    first = jnp.concatenate([fields[0, :3], fields[1, :3], fields[2, :2]], axis=0)
    cost = pl.CostEstimate(flops=100_000_000, bytes_accessed=1_000_000, transcendentals=0)
    params = pltpu.CompilerParams(vmem_limit_bytes=16 * 1024 * 1024)
    now, first, last = pl.pallas_call(
        first_step_kernel,
        out_shape=(
            jax.ShapeDtypeStruct((3, rows, members, columns), f32),
            jax.ShapeDtypeStruct((8, members, columns), bf16),
            jax.ShapeDtypeStruct((8, members, columns), bf16),
        ),
        in_specs=[vmem] * 3,
        out_specs=(vmem,) * 3,
        compiler_params=params,
        cost_estimate=cost,
        name="step_one",
    )(fields, lax.ppermute(last, "space", up), lax.ppermute(first, "space", down))
    return pl.pallas_call(
        last_step_kernel,
        out_shape=jax.ShapeDtypeStruct((columns // 64, members, COLS), bf16),
        in_specs=[vmem] * 3,
        out_specs=vmem,
        compiler_params=params,
        cost_estimate=cost,
        name="step_two",
    )(now, lax.ppermute(last, "space", up), lax.ppermute(first, "space", down))


def dot(a, b):
    return jnp.dot(a, b, preferred_element_type=f32)


def dot_t(a, b):
    return lax.dot_general(a, b, (((1,), (1,)), ((), ())), preferred_element_type=f32)


def split(a):
    high = a.astype(bf16)
    return high, (a - high.astype(f32)).astype(bf16)


def product(a, b):
    return dot(a[0], b[0]) + (dot(a[0], b[1]) + dot(a[1], b[0]))


def eye(n):
    return (
        lax.broadcasted_iota(jnp.int32, (n, n), 0) == lax.broadcasted_iota(jnp.int32, (n, n), 1)
    ).astype(f32)


def total(a):
    return jnp.sum(jnp.sum(a, axis=1, keepdims=True), axis=0, keepdims=True)


def weights_kernel(
    region, index_row, index_col, value_row, var_row, var_col, packed, z_ref, zt_ref, b_ref, m_ref, l_ref, u_ref
):
    own = jnp.concatenate([region[:, :BLOCK], region[:, HALF : HALF + BLOCK]], axis=1)
    cell_row = lax.broadcasted_iota(jnp.int32, (CELLS, OBS), 0)
    pick = (cell_row == index_row[...]).astype(f32).astype(bf16)
    cell_col = lax.broadcasted_iota(jnp.int32, (OBS, CELLS), 1)
    pick_t = (cell_col == index_col[...]).astype(f32).astype(bf16)
    y = dot(own, pick)
    mean_row = jnp.sum(y, axis=0, keepdims=True) * (1.0 / MEMBERS)
    inverse_row = lax.rsqrt(var_row[...])
    z_ref[...] = (y - mean_row) * inverse_row
    y_t = dot_t(pick_t, own)
    mean_col = jnp.sum(y_t, axis=1, keepdims=True) * (1.0 / MEMBERS)
    zt_ref[...] = (y_t - mean_col) * lax.rsqrt(var_col[...])
    w_row = (value_row[...] - mean_row) * inverse_row

    b = product(split(zt_ref[...]), split(z_ref[...]))
    identity = eye(OBS)
    diagonal = float(MEMBERS - 1)
    squared = diagonal * diagonal * MEMBERS + 2.0 * diagonal * total(b * identity) + total(b * b)
    inverse_norm = lax.rsqrt(squared)
    alpha = diagonal * inverse_norm
    b = b * inverse_norm
    b_ref[...] = b

    low = 1.5 - 0.5 * alpha
    lower = low * identity - 0.5 * b
    l_ref[...] = lower
    u_ref[...] = alpha * lower + product(split(b), split(lower))
    m_ref[...] = -0.5 * identity

    def step_parts(low):
        m = m_ref[...]
        lower = l_ref[...]
        crossed = product(split(m), split(u_ref[...]))
        part = -0.5 * (low * (alpha * m + lower) + crossed)
        factor = 1.5 - 0.5 * alpha * low * low
        return factor * m + product(split(part), split(lower)), factor * low

    def one_step(_, low):
        m, low = step_parts(low)
        m_ref[...] = m
        b_parts = split(b_ref[...])
        lower = low * eye(OBS) + product(split(m), b_parts)
        l_ref[...] = lower
        u_ref[...] = alpha * lower + product(b_parts, split(lower))
        return low

    low = lax.fori_loop(0, NS_STEPS - 2, one_step, low)
    m, low = step_parts(low)

    b = b_ref[...]
    once = low * w_row + jnp.sum(
        m * jnp.sum(b * w_row, axis=1, keepdims=True), axis=0, keepdims=True
    )
    inner = jnp.sum(b * once, axis=1, keepdims=True)
    once_col = jnp.sum(identity * once, axis=1, keepdims=True)
    inner_row = jnp.sum(identity * inner, axis=0, keepdims=True)
    twice = low * once_col + jnp.sum(m * inner_row, axis=1, keepdims=True)
    centre = jnp.sum(zt_ref[...] * twice, axis=0, keepdims=True) * inverse_norm

    scale = math.sqrt(diagonal) * jnp.sqrt(inverse_norm)
    m_parts = split(m * (scale * inverse_norm))
    small = eye(BLOCK)
    spot = lax.broadcasted_iota(jnp.int32, (16, BLOCK), 0)
    at = 0
    for i in range(4):
        v = product(split(z_ref[i * BLOCK : (i + 1) * BLOCK, :]), m_parts)
        band = product(split(v), split(zt_ref[:, i * BLOCK :]))
        for j in range(i, 4):
            block = band[:, (j - i) * BLOCK : (j - i + 1) * BLOCK]
            if i == j:
                block = block + (scale * low) * small
            packed[at : at + BLOCK, :] = block.astype(bf16)
            at += BLOCK
        piece = centre[:, i * BLOCK : (i + 1) * BLOCK]
        high = piece.astype(bf16).astype(f32)
        both = jnp.where(spot == 0, high, jnp.where(spot == 1, piece - high, 0.0))
        start = CENTRE_AT + 16 * i
        packed[start : start + 16, :] = both.astype(bf16)


def region_weights(region, index, values, variances):
    return pl.pallas_call(
        weights_kernel,
        out_shape=jax.ShapeDtypeStruct((PACKED, BLOCK), bf16),
        in_specs=[pl.BlockSpec(memory_space=pltpu.VMEM)] * 6,
        out_specs=pl.BlockSpec(memory_space=pltpu.VMEM),
        scratch_shapes=[
            pltpu.VMEM((MEMBERS, OBS), f32),
            pltpu.VMEM((OBS, MEMBERS), f32),
            pltpu.VMEM((OBS, OBS), f32),
            pltpu.VMEM((OBS, OBS), f32),
            pltpu.VMEM((OBS, OBS), f32),
            pltpu.VMEM((OBS, OBS), f32),
        ],
        compiler_params=pltpu.CompilerParams(vmem_limit_bytes=24 * 1024 * 1024),
        cost_estimate=pl.CostEstimate(flops=6_000_000_000, bytes_accessed=1_000_000, transcendentals=0),
        name="weights",
    )(
        region,
        index.reshape(1, OBS),
        index.reshape(OBS, 1),
        values.reshape(1, OBS),
        variances.reshape(1, OBS),
        variances.reshape(OBS, 1),
    )


def column_parts(columns, parity):
    place = lax.broadcasted_iota(jnp.int32, (1, columns), 1)
    row = 2 * (place // HALF) + (place // 64) % 2
    col = place % 64
    row_weight = jnp.abs((row.astype(f32) + 0.5) / 4.0 - 0.5)
    col_weight = jnp.abs((col.astype(f32) + 0.5) / 64.0 - 0.5)
    right = (col >= 32).astype(jnp.int32)
    sibling = ((right + parity) == 1).astype(f32)
    return row_weight, col_weight, sibling


def factors(parity):
    r, q, sibling = column_parts(COLS, parity)
    side = {0: 1.0 - q, 1: q * sibling, 2: q * (1.0 - sibling)}
    return {(row, s): (r if row else 1.0 - r) * side[s] for row in (0, 1) for s in (0, 1, 2)}


def unpack(source, base, full):
    for n, (i, j) in enumerate(PAIRS):
        block = source[base + n * BLOCK : base + (n + 1) * BLOCK, :]
        full[i * BLOCK : (i + 1) * BLOCK, j * BLOCK : (j + 1) * BLOCK] = block
        if i != j:
            turned = jnp.transpose(block.astype(f32)).astype(bf16)
            full[j * BLOCK : (j + 1) * BLOCK, i * BLOCK : (i + 1) * BLOCK] = turned


def apply(source, base, full, dev, acc, lo, hi, factor, first, out=None):
    unpack(source, base, full)
    shift = jnp.zeros((16, hi - lo), f32)
    for i in range(4):
        start = base + CENTRE_AT + 16 * i
        shift = shift + dot(source[start : start + 16, :], dev[i * BLOCK : (i + 1) * BLOCK, lo:hi])
    shift = jnp.sum(shift, axis=0, keepdims=True)
    factor = factor[:, lo:hi]

    def rows(i, carry):
        at = pl.ds(pl.multiple_of(i * BLOCK, BLOCK), BLOCK)
        term = factor * (dot(full[at, :], dev[:, lo:hi]) + shift)
        if not first:
            term = term + acc[at, lo:hi]
        if out is None:
            acc[at, lo:hi] = term
        else:
            out[at, lo:hi] = term.astype(bf16)
        return carry

    lax.fori_loop(0, 4, rows, 0)


def near_kernel(parity, region, own, sibling, other, below, above, acc, dev, full, mean_ref):
    for g in range(COLS // BLOCK):
        at = slice(g * BLOCK, (g + 1) * BLOCK)
        part = region[:, at].astype(f32)
        mean = jnp.sum(part, axis=0, keepdims=True) * (1.0 / MEMBERS)
        mean_ref[:, at] = mean
        dev[:, at] = (part - mean).astype(bf16)
    factor = factors(parity[0])
    apply(own, 0, full, dev, acc, 0, COLS, factor[0, 0], True)
    apply(sibling, 0, full, dev, acc, 0, COLS, factor[0, 1], False)
    apply(other, 0, full, dev, acc, 0, COLS, factor[0, 2], False)
    apply(below, 0, full, dev, acc, 0, HALF, factor[1, 0], False)
    apply(above, 0, full, dev, acc, HALF, COLS, factor[1, 0], False)
    acc[...] = acc[...] + mean_ref[...]


def far_kernel(parity, acc, dev, siblings, below_other, above_other, out, scratch, full):
    factor = factors(parity[0])
    scratch[...] = acc[...]
    apply(siblings, 0, full, dev, scratch, 0, HALF, factor[1, 1], False)
    apply(siblings, PACKED, full, dev, scratch, HALF, COLS, factor[1, 1], False)
    apply(below_other, 0, full, dev, scratch, 0, HALF, factor[1, 2], False, out)
    apply(above_other, 0, full, dev, scratch, HALF, COLS, factor[1, 2], False, out)


def blend_near(parity, region, own, sibling, other, below, above):
    return pl.pallas_call(
        near_kernel,
        out_shape=(
            jax.ShapeDtypeStruct((MEMBERS, COLS), f32),
            jax.ShapeDtypeStruct((MEMBERS, COLS), bf16),
        ),
        in_specs=[smem] + [vmem] * 6,
        out_specs=(vmem, vmem),
        scratch_shapes=[pltpu.VMEM((MEMBERS, MEMBERS), bf16), pltpu.VMEM((1, COLS), f32)],
        compiler_params=pltpu.CompilerParams(vmem_limit_bytes=24 * 1024 * 1024),
        cost_estimate=pl.CostEstimate(flops=1_600_000_000, bytes_accessed=1_000_000, transcendentals=0),
        name="near",
    )(parity, region, own, sibling, other, below, above)


def blend_far(parity, acc, dev, siblings, below_other, above_other):
    return pl.pallas_call(
        far_kernel,
        out_shape=jax.ShapeDtypeStruct((MEMBERS, COLS), bf16),
        in_specs=[smem] + [vmem] * 5,
        out_specs=vmem,
        scratch_shapes=[pltpu.VMEM((MEMBERS, COLS), f32), pltpu.VMEM((MEMBERS, MEMBERS), bf16)],
        compiler_params=pltpu.CompilerParams(vmem_limit_bytes=24 * 1024 * 1024),
        cost_estimate=pl.CostEstimate(flops=800_000_000, bytes_accessed=1_000_000, transcendentals=0),
        name="far",
    )(parity, acc, dev, siblings, below_other, above_other)


def per_device(ensemble, obs_index, obs_value, obs_var):
    bands = lax.axis_size("space")
    tiles = lax.axis_size("member")
    tile = lax.axis_index("member")
    up = [(i, (i + 1) % bands) for i in range(bands)]
    down = [(j, i) for i, j in up]
    sibling_pairs = [(i, i ^ 1) for i in range(tiles)]
    other_pairs = [(i, (i + 1) % tiles if i % 2 else (i - 1) % tiles) for i in range(tiles)]

    chunks = forecast(ensemble[0].transpose(1, 2, 0, 3), up, down)
    near_members = chunks.shape[1]
    region = lax.all_to_all(chunks, "member", 0, 0, tiled=True).reshape(MEMBERS, COLS)
    index = lax.dynamic_index_in_dim(obs_index[0, 0], tile, 0, keepdims=False)
    own = region_weights(region, index, obs_value[0, 0, 0], obs_var[0, 0, 0])
    below = lax.ppermute(own, "space", up)
    above = lax.ppermute(own, "space", down)
    other = lax.ppermute(own, "member", other_pairs)
    sibling = lax.ppermute(own, "member", sibling_pairs)
    below_other = lax.ppermute(other, "space", up)
    above_other = lax.ppermute(other, "space", down)
    siblings = lax.ppermute(jnp.concatenate([below, above]), "member", sibling_pairs)
    parity = (tile % 2).astype(jnp.int32).reshape(1)
    acc, dev = blend_near(parity, region, own, sibling, other, below, above)
    analysed = blend_far(parity, acc, dev, siblings, below_other, above_other)
    back = lax.all_to_all(
        analysed.reshape(tiles, near_members, COLS), "member", 0, 0, tiled=True
    )
    back = back.reshape(tiles, near_members, 2, 3, 2, 64).transpose(1, 3, 2, 4, 0, 5)
    return back.reshape(1, near_members, 3, 4, tiles * 64)


def solution(mesh):
    return jax.shard_map(
        per_device,
        mesh=mesh,
        in_specs=(
            P("group", "member", None, "space", None),
            P("group", "space", None, None),
            P("group", "space", "member", None),
            P("group", "space", "member", None),
        ),
        out_specs=P("group", "member", None, "space", None),
        check_vma=False,
    )
```

```python
import functools
import math

import jax
import jax.numpy as jnp
from jax import lax
from jax.experimental import pallas as pl
from jax.experimental.pallas import tpu as pltpu
from jax.sharding import PartitionSpec as P

NS_STEPS = 6
MEMBERS = 512
CELLS = 256
OBS = 256
BLOCK = 128
PAIRS = [(i, j) for i in range(4) for j in range(i, 4)]
CENTRE_AT = len(PAIRS) * BLOCK
PACKED = CENTRE_AT + 4 * 16

time_step = 0.4
coriolis = 0.3
COLS = 768
HALF = 384
HALVES = 1
PARTS = 2
f32 = jnp.float32
bf16 = jnp.bfloat16
vmem = pl.BlockSpec(memory_space=pltpu.VMEM)
smem = pl.BlockSpec(memory_space=pltpu.SMEM)


def column_difference(field):
    columns = field.shape[-1]
    return 0.5 * (pltpu.roll(field, columns - 1, 1) - pltpu.roll(field, 1, 1))


def rates(h, v, u, i):
    d_height = -(column_difference(u[i]) + 0.5 * (v[i + 1] - v[i - 1]))
    d_north = -0.5 * (h[i + 1] - h[i - 1]) - coriolis * u[i]
    return d_height, d_north


def rate_east(h, v, i):
    return coriolis * v[i] - column_difference(h[i])


def advance(h0, v0, u0):
    h1, v1, u1, h2, v2, u2, h3, v3, u3 = ({} for _ in range(9))
    for i in range(-2, 6):
        dh, dv = rates(h0, v0, u0, i)
        h1[i] = h0[i] + time_step * dh
        v1[i] = v0[i] + time_step * dv
        if -1 <= i <= 4:
            u1[i] = u0[i] + time_step * rate_east(h0, v0, i)
    for i in range(-1, 5):
        dh, dv = rates(h1, v1, u1, i)
        h2[i] = 0.75 * h0[i] + 0.25 * (h1[i] + time_step * dh)
        v2[i] = 0.75 * v0[i] + 0.25 * (v1[i] + time_step * dv)
        if 0 <= i <= 3:
            u2[i] = 0.75 * u0[i] + 0.25 * (u1[i] + time_step * rate_east(h1, v1, i))
    third = 1.0 / 3.0
    two_thirds = 2.0 / 3.0
    for i in range(4):
        dh, dv = rates(h2, v2, u2, i)
        h3[i] = h0[i] * third + two_thirds * (h2[i] + time_step * dh)
        v3[i] = v0[i] * third + two_thirds * (v2[i] + time_step * dv)
        u3[i] = u0[i] * third + two_thirds * (u2[i] + time_step * rate_east(h2, v2, i))
    return h3, v3, u3


GROUP = 16


def loaded(now, below, above, at):
    h, v, u = {}, {}, {}
    for f, field in enumerate((h, v, u)):
        for i in range(4):
            field[i] = now[f, i, at, :].astype(f32)
    for k in range(3):
        h[k - 3] = below[k, at, :].astype(f32)
        v[k - 3] = below[3 + k, at, :].astype(f32)
        h[4 + k] = above[k, at, :].astype(f32)
        v[4 + k] = above[3 + k, at, :].astype(f32)
    for k in range(2):
        u[k - 2] = below[6 + k, at, :].astype(f32)
        u[4 + k] = above[6 + k, at, :].astype(f32)
    return h, v, u


def first_step_kernel(now, below, above, out, first, last):
    def group(g, carry):
        at = pl.ds(pl.multiple_of(g * GROUP, GROUP), GROUP)
        fields = advance(*loaded(now, below, above, at))
        for f in range(3):
            edge = 2 if f == 2 else 3
            for i in range(4):
                out[f, i, at, :] = fields[f][i]
                if i < edge:
                    first[3 * f + i, at, :] = fields[f][i].astype(bf16)
                if i >= 4 - edge:
                    last[3 * f + i - (4 - edge), at, :] = fields[f][i].astype(bf16)
        return carry

    lax.fori_loop(0, now.shape[2] // GROUP, group, 0)


def last_step_kernel(base, now, below, above, *refs):
    out = refs[-1]
    lane = lax.broadcasted_iota(jnp.int32, (GROUP, BLOCK), 1) < 64

    def group(g, carry):
        at = pl.ds(pl.multiple_of(g * GROUP, GROUP), GROUP)
        into = pl.ds(pl.multiple_of(base + g * GROUP, GROUP), GROUP)
        fields = advance(*loaded(now, below, above, at))
        for f in range(3):
            for p in range(2):
                to = p * HALF + f * BLOCK
                for t in range(4):
                    x = fields[f][2 * p][:, t * BLOCK : (t + 1) * BLOCK]
                    y = fields[f][2 * p + 1][:, t * BLOCK : (t + 1) * BLOCK]
                    even = jnp.where(lane, x, pltpu.roll(y, 64, 1))
                    odd = jnp.where(lane, pltpu.roll(x, 64, 1), y)
                    out[2 * t, into, to : to + BLOCK] = even.astype(bf16)
                    out[2 * t + 1, into, to : to + BLOCK] = odd.astype(bf16)
        return carry

    lax.fori_loop(0, now.shape[2] // GROUP, group, 0)


def swapped(last, first, up, down):
    return lax.ppermute(last, "space", up), lax.ppermute(first, "space", down)


def edges(fields):
    last = jnp.concatenate([fields[0, 1:], fields[1, 1:], fields[2, 2:]], axis=0)
    first = jnp.concatenate([fields[0, :3], fields[1, :3], fields[2, :2]], axis=0)
    return last, first


def step(kernel, outs, *arrays, aliases={}):
    return pl.pallas_call(
        kernel,
        out_shape=outs,
        in_specs=[vmem] * len(arrays),
        out_specs=jax.tree.map(lambda _: vmem, outs),
        input_output_aliases=aliases,
        compiler_params=pltpu.CompilerParams(vmem_limit_bytes=12 * 1024 * 1024),
        cost_estimate=pl.CostEstimate(
            flops=100_000_000 // PARTS, bytes_accessed=1_000_000, transcendentals=0
        ),
    )(*arrays)


def forecast(fields, up, down):
    _, rows, members, columns = fields.shape
    half = members // PARTS
    now_shape = jax.ShapeDtypeStruct((3, rows, half, columns), f32)
    edge_shape = jax.ShapeDtypeStruct((8, half, columns), bf16)
    chunk_shape = jax.ShapeDtypeStruct((columns // 64, members, COLS), bf16)
    parts = [fields[:, :, n * half : (n + 1) * half] for n in range(PARTS)]
    halos = [swapped(*edges(part), up, down) for part in parts]
    first_outs = (now_shape, edge_shape, edge_shape)
    chunks = ()
    for n in range(PARTS):
        now, first, last = step(first_step_kernel, first_outs, parts[n], *halos[n])
        halo = swapped(last, first, up, down)
        kernel = functools.partial(last_step_kernel, n * half)
        aliases = {3: 0} if chunks else {}
        chunks = (step(kernel, chunk_shape, now, *halo, *chunks, aliases=aliases),)
    return chunks[0]


def dot(a, b):
    return jnp.dot(a, b, preferred_element_type=f32)


def dot_t(a, b):
    return lax.dot_general(a, b, (((1,), (1,)), ((), ())), preferred_element_type=f32)


def split(a):
    high = a.astype(bf16)
    return high, (a - high.astype(f32)).astype(bf16)


def product(a, b):
    return dot(a[0], b[0]) + (dot(a[0], b[1]) + dot(a[1], b[0]))


def eye(n):
    return (
        lax.broadcasted_iota(jnp.int32, (n, n), 0) == lax.broadcasted_iota(jnp.int32, (n, n), 1)
    ).astype(f32)


def total(a):
    return jnp.sum(jnp.sum(a, axis=1, keepdims=True), axis=0, keepdims=True)


def weights_kernel(*refs):
    regions = refs[:HALVES]
    tile, index, value, var, packed = refs[HALVES : HALVES + 5]
    z_ref, zt_ref, b_ref, m_ref, l_ref, u_ref = refs[HALVES + 5 :]
    identity = eye(OBS)

    def as_column(row):
        return jnp.sum(identity * row, axis=1, keepdims=True)

    index_row = index[pl.ds(tile[0], 1), :]
    index_col = as_column(index_row.astype(f32)).astype(jnp.int32)
    var_row = var[...]
    var_col = as_column(var_row)
    own = jnp.concatenate(
        [
            jnp.concatenate([part[:, :BLOCK], part[:, HALF : HALF + BLOCK]], axis=1)
            for part in regions
        ],
        axis=0,
    )
    cell_row = lax.broadcasted_iota(jnp.int32, (CELLS, OBS), 0)
    pick = (cell_row == index_row).astype(f32).astype(bf16)
    cell_col = lax.broadcasted_iota(jnp.int32, (OBS, CELLS), 1)
    pick_t = (cell_col == index_col).astype(f32).astype(bf16)
    y = dot(own, pick)
    mean_row = jnp.sum(y, axis=0, keepdims=True) * (1.0 / MEMBERS)
    inverse_row = lax.rsqrt(var_row)
    z_ref[...] = (y - mean_row) * inverse_row
    y_t = dot_t(pick_t, own)
    mean_col = jnp.sum(y_t, axis=1, keepdims=True) * (1.0 / MEMBERS)
    zt_ref[...] = (y_t - mean_col) * lax.rsqrt(var_col)
    w_row = (value[...] - mean_row) * inverse_row

    b = product(split(zt_ref[...]), split(z_ref[...]))
    diagonal = float(MEMBERS - 1)
    squared = diagonal * diagonal * MEMBERS + 2.0 * diagonal * total(b * identity) + total(b * b)
    inverse_norm = lax.rsqrt(squared)
    alpha = diagonal * inverse_norm
    b = b * inverse_norm
    b_ref[...] = b

    low = 1.5 - 0.5 * alpha
    lower = low * identity - 0.5 * b
    l_ref[...] = lower
    u_ref[...] = alpha * lower + product(split(b), split(lower))
    m_ref[...] = -0.5 * identity

    def one_step(_, low):
        identity = eye(OBS)
        m = m_ref[...]
        lower = l_ref[...]
        l_parts = split(lower)
        u_parts = split(u_ref[...])
        step = split(1.5 * identity - 0.5 * product(l_parts, u_parts))
        part = split(-0.5 * (low * (alpha * m + lower) + product(split(m), u_parts)))
        factor = 1.5 - 0.5 * alpha * low * low
        l_ref[...] = product(step, l_parts)
        m_ref[...] = factor * m + product(part, l_parts)
        u_ref[...] = product(step, u_parts)
        return factor * low

    low = lax.fori_loop(0, NS_STEPS - 2, one_step, low)
    m = m_ref[...]
    lower = l_ref[...]
    part = -0.5 * (low * (alpha * m + lower) + product(split(m), split(u_ref[...])))
    factor = 1.5 - 0.5 * alpha * low * low
    m = factor * m + product(split(part), split(lower))
    low = factor * low

    b = b_ref[...]
    once = low * w_row + jnp.sum(
        m * jnp.sum(b * w_row, axis=1, keepdims=True), axis=0, keepdims=True
    )
    inner = jnp.sum(b * once, axis=1, keepdims=True)
    once_col = jnp.sum(identity * once, axis=1, keepdims=True)
    inner_row = jnp.sum(identity * inner, axis=0, keepdims=True)
    twice = low * once_col + jnp.sum(m * inner_row, axis=1, keepdims=True)
    centre = jnp.sum(zt_ref[...] * twice, axis=0, keepdims=True) * inverse_norm

    scale = math.sqrt(diagonal) * jnp.sqrt(inverse_norm)
    m_parts = split(m * (scale * inverse_norm))
    small = eye(BLOCK)
    spot = lax.broadcasted_iota(jnp.int32, (16, BLOCK), 0)
    at = 0
    for i in range(4):
        v = product(split(z_ref[i * BLOCK : (i + 1) * BLOCK, :]), m_parts)
        band = product(split(v), split(zt_ref[:, i * BLOCK :]))
        for j in range(i, 4):
            block = band[:, (j - i) * BLOCK : (j - i + 1) * BLOCK]
            if i == j:
                block = block + (scale * low) * small
            packed[at : at + BLOCK, :] = block.astype(bf16)
            at += BLOCK
        piece = centre[:, i * BLOCK : (i + 1) * BLOCK]
        high = piece.astype(bf16).astype(f32)
        both = jnp.where(spot == 0, high, jnp.where(spot == 1, piece - high, 0.0))
        start = CENTRE_AT + 16 * i
        packed[start : start + 16, :] = both.astype(bf16)


def region_weights(regions, tile, index, values, variances):
    return pl.pallas_call(
        weights_kernel,
        out_shape=jax.ShapeDtypeStruct((PACKED, BLOCK), bf16),
        in_specs=[vmem] * HALVES + [smem] + [vmem] * 3,
        out_specs=pl.BlockSpec(memory_space=pltpu.VMEM),
        scratch_shapes=[
            pltpu.VMEM((MEMBERS, OBS), f32),
            pltpu.VMEM((OBS, MEMBERS), f32),
            pltpu.VMEM((OBS, OBS), f32),
            pltpu.VMEM((OBS, OBS), f32),
            pltpu.VMEM((OBS, OBS), f32),
            pltpu.VMEM((OBS, OBS), f32),
        ],
        compiler_params=pltpu.CompilerParams(vmem_limit_bytes=24 * 1024 * 1024),
        cost_estimate=pl.CostEstimate(flops=6_000_000_000, bytes_accessed=1_000_000, transcendentals=0),
        name="weights",
    )(
        *regions,
        tile,
        index,
        values,
        variances,
    )


def column_parts(columns, parity):
    place = lax.broadcasted_iota(jnp.int32, (1, columns), 1)
    row = 2 * (place // HALF) + (place // 64) % 2
    col = place % 64
    row_weight = jnp.abs((row.astype(f32) + 0.5) / 4.0 - 0.5)
    col_weight = jnp.abs((col.astype(f32) + 0.5) / 64.0 - 0.5)
    right = (col >= 32).astype(jnp.int32)
    sibling = ((right + parity) == 1).astype(f32)
    return row_weight, col_weight, sibling


def factors(parity):
    r, q, sibling = column_parts(COLS, parity)
    side = {0: 1.0 - q, 1: q * sibling, 2: q * (1.0 - sibling)}
    return {(row, s): (r if row else 1.0 - r) * side[s] for row in (0, 1) for s in (0, 1, 2)}


def unpack(source, base, full):
    for n, (i, j) in enumerate(PAIRS):
        block = source[base + n * BLOCK : base + (n + 1) * BLOCK, :]
        full[i * BLOCK : (i + 1) * BLOCK, j * BLOCK : (j + 1) * BLOCK] = block
        if i != j:
            turned = jnp.transpose(block.astype(f32)).astype(bf16)
            full[j * BLOCK : (j + 1) * BLOCK, i * BLOCK : (i + 1) * BLOCK] = turned


def apply(source, base, full, dev, acc, lo, hi, factor, before=None, out=None):
    unpack(source, base, full)
    shift = jnp.zeros((16, hi - lo), f32)
    for i in range(4):
        start = base + CENTRE_AT + 16 * i
        shift = shift + dot(source[start : start + 16, :], dev[i * BLOCK : (i + 1) * BLOCK, lo:hi])
    shift = jnp.sum(shift, axis=0, keepdims=True)
    factor = factor[:, lo:hi]
    wide = MEMBERS // HALVES // BLOCK
    slots = BLOCK * 8 // (MEMBERS // HALVES)
    size = BLOCK // slots

    def rows(i, carry):
        at = pl.ds(pl.multiple_of(i * BLOCK, BLOCK), BLOCK)
        term = factor * (dot(full[at, :], dev[:, lo:hi]) + shift)
        term = term + (acc[at, lo:hi] if before is None else before[:, lo:hi])
        if out is None:
            acc[at, lo:hi] = term
        else:
            tiles = pl.ds((i % wide) * slots, slots)
            spot = pl.ds(pl.multiple_of((i // wide) * size, size), size)
            out[tiles, spot, lo:hi] = term.astype(bf16).reshape(slots, size, hi - lo)
        return carry

    lax.fori_loop(0, 4, rows, 0)


def own_kernel(*refs):
    parity = refs[0]
    regions = refs[1 : 1 + HALVES]
    own, acc, dev, full, mean_ref = refs[1 + HALVES :]
    size = MEMBERS // HALVES
    for g in range(COLS // BLOCK):
        at = slice(g * BLOCK, (g + 1) * BLOCK)
        parts = [part[:, at].astype(f32) for part in regions]
        mean = sum(jnp.sum(part, axis=0, keepdims=True) for part in parts) * (1.0 / MEMBERS)
        mean_ref[:, at] = mean
        for n, part in enumerate(parts):
            dev[n * size : (n + 1) * size, at] = (part - mean).astype(bf16)
    apply(own, 0, full, dev, acc, 0, COLS, factors(parity[0])[0, 0], before=mean_ref)


def near_kernel(parity, acc_in, dev, sibling, other, below, above, acc, full):
    factor = factors(parity[0])
    apply(sibling, 0, full, dev, acc, 0, COLS, factor[0, 1])
    apply(other, 0, full, dev, acc, 0, COLS, factor[0, 2])
    apply(below, 0, full, dev, acc, 0, HALF, factor[1, 0])
    apply(above, 0, full, dev, acc, HALF, COLS, factor[1, 0])


def side_kernel(parity, acc_in, dev, below_sibling, above_sibling, acc, full):
    factor = factors(parity[0])
    apply(below_sibling, 0, full, dev, acc, 0, HALF, factor[1, 1])
    apply(above_sibling, 0, full, dev, acc, HALF, COLS, factor[1, 1])


def far_kernel(parity, acc, dev, below_other, above_other, out, full):
    factor = factors(parity[0])
    apply(below_other, 0, full, dev, acc, 0, HALF, factor[1, 2], out=out)
    apply(above_other, 0, full, dev, acc, HALF, COLS, factor[1, 2], out=out)


def call(kernel, outs, flops, scratch, parity, *arrays, alias=False):
    return pl.pallas_call(
    kernel,
    out_shape=outs,
    in_specs=[smem] + [vmem] * len(arrays),
    out_specs=jax.tree.map(lambda _: vmem, outs),
    scratch_shapes=[pltpu.VMEM((MEMBERS, MEMBERS), bf16)] + scratch,
    input_output_aliases={1: 0} if alias else {},
    compiler_params=pltpu.CompilerParams(vmem_limit_bytes=16 * 1024 * 1024),
    cost_estimate=pl.CostEstimate(flops=flops, bytes_accessed=1_000_000, transcendentals=0),
    )(parity, *arrays)


def program(ensemble, obs_index, obs_value, obs_var):
    bands = lax.axis_size("space")
    tiles = lax.axis_size("member")
    tile = lax.axis_index("member")
    up = [(i, (i + 1) % bands) for i in range(bands)]
    down = [(j, i) for i, j in up]
    sibling_pairs = [(i, i ^ 1) for i in range(tiles)]
    other_pairs = [(i, (i + 1) % tiles if i % 2 else (i - 1) % tiles) for i in range(tiles)]

    near_members = ensemble.shape[1]
    fields, tile = lax.optimization_barrier((ensemble[0].transpose(1, 2, 0, 3), tile))
    parity = (tile % 2).astype(jnp.int32).reshape(1)
    chunks = forecast(fields, up, down)
    region = lax.all_to_all(chunks, "member", 0, 0, tiled=True).reshape(MEMBERS, COLS)
    regions = [region]
    own = region_weights(regions, tile.reshape(1), obs_index[0, 0], obs_value[0, 0], obs_var[0, 0])

    other = lax.ppermute(own, "member", other_pairs)
    below = lax.ppermute(own, "space", up)
    above = lax.ppermute(own, "space", down)
    sibling = lax.ppermute(own, "member", sibling_pairs)
    below_other = lax.ppermute(other, "space", up)
    above_other = lax.ppermute(other, "space", down)
    below_sibling = lax.ppermute(below, "member", sibling_pairs)
    above_sibling = lax.ppermute(above, "member", sibling_pairs)
    total_shape = jax.ShapeDtypeStruct((MEMBERS, COLS), f32)
    dev_shape = jax.ShapeDtypeStruct((MEMBERS, COLS), bf16)
    out_shape = jax.ShapeDtypeStruct((tiles, near_members, COLS), bf16)
    mean_scratch = [pltpu.VMEM((1, COLS), f32)]
    acc, dev = call(own_kernel, (total_shape, dev_shape), 400_000_000, mean_scratch, parity, *regions, own)
    acc = call(near_kernel, total_shape, 1_200_000_000, [], parity, acc, dev, sibling, other, below, above, alias=True)
    acc = call(side_kernel, total_shape, 400_000_000, [], parity, acc, dev, below_sibling, above_sibling, alias=True)
    analysed = call(far_kernel, out_shape, 400_000_000, [], parity, acc, dev, below_other, above_other)
    back = lax.all_to_all(analysed, "member", 0, 0, tiled=True)
    back = back.reshape(tiles, near_members, 2, 3, 2, 64).transpose(1, 3, 2, 4, 0, 5)
    return back.reshape(1, near_members, 3, 4, tiles * 64)


def solution(mesh):
    return jax.shard_map(
        program,
        mesh=mesh,
        in_specs=(
            P("group", "member", None, "space", None),
            P("group", "space", None, None),
            P("group", "space", "member", None),
            P("group", "space", "member", None),
        ),
        out_specs=P("group", "member", None, "space", None),
        check_vma=False,
    )
```

```python
import functools
import math

import jax
import jax.numpy as jnp
from jax import lax
from jax.experimental import pallas as pl
from jax.experimental.pallas import tpu as pltpu
from jax.sharding import PartitionSpec as P

NS_STEPS = 6
MEMBERS = 512
CELLS = 256
OBS = 256
BLOCK = 128
PAIRS = [(i, j) for i in range(4) for j in range(i, 4)]
CENTRE_AT = len(PAIRS) * BLOCK
FRONT = len(PAIRS) // 2 * BLOCK
PACKED = CENTRE_AT + 4 * 16

time_step = 0.4
coriolis = 0.3
COLS = 768
HALF = 384
HALVES = 1
PARTS = 2
f32 = jnp.float32
bf16 = jnp.bfloat16
vmem = pl.BlockSpec(memory_space=pltpu.VMEM)
smem = pl.BlockSpec(memory_space=pltpu.SMEM)


def column_difference(field):
    columns = field.shape[-1]
    return 0.5 * (pltpu.roll(field, columns - 1, 1) - pltpu.roll(field, 1, 1))


def rates(h, v, u, i):
    d_height = -(column_difference(u[i]) + 0.5 * (v[i + 1] - v[i - 1]))
    d_north = -0.5 * (h[i + 1] - h[i - 1]) - coriolis * u[i]
    return d_height, d_north


def rate_east(h, v, i):
    return coriolis * v[i] - column_difference(h[i])


def advance(h0, v0, u0):
    h1, v1, u1, h2, v2, u2, h3, v3, u3 = ({} for _ in range(9))
    for i in range(-2, 6):
        dh, dv = rates(h0, v0, u0, i)
        h1[i] = h0[i] + time_step * dh
        v1[i] = v0[i] + time_step * dv
        if -1 <= i <= 4:
            u1[i] = u0[i] + time_step * rate_east(h0, v0, i)
    for i in range(-1, 5):
        dh, dv = rates(h1, v1, u1, i)
        h2[i] = 0.75 * h0[i] + 0.25 * (h1[i] + time_step * dh)
        v2[i] = 0.75 * v0[i] + 0.25 * (v1[i] + time_step * dv)
        if 0 <= i <= 3:
            u2[i] = 0.75 * u0[i] + 0.25 * (u1[i] + time_step * rate_east(h1, v1, i))
    third = 1.0 / 3.0
    two_thirds = 2.0 / 3.0
    for i in range(4):
        dh, dv = rates(h2, v2, u2, i)
        h3[i] = h0[i] * third + two_thirds * (h2[i] + time_step * dh)
        v3[i] = v0[i] * third + two_thirds * (v2[i] + time_step * dv)
        u3[i] = u0[i] * third + two_thirds * (u2[i] + time_step * rate_east(h2, v2, i))
    return h3, v3, u3


GROUP = 16


def loaded(now, below, above, at):
    h, v, u = {}, {}, {}
    for f, field in enumerate((h, v, u)):
        for i in range(4):
            field[i] = now[f, i, at, :].astype(f32)
    for k in range(3):
        h[k - 3] = below[k, at, :].astype(f32)
        v[k - 3] = below[3 + k, at, :].astype(f32)
        h[4 + k] = above[k, at, :].astype(f32)
        v[4 + k] = above[3 + k, at, :].astype(f32)
    for k in range(2):
        u[k - 2] = below[6 + k, at, :].astype(f32)
        u[4 + k] = above[6 + k, at, :].astype(f32)
    return h, v, u


def first_step_kernel(now, below, above, out, first, last):
    def group(g, carry):
        at = pl.ds(pl.multiple_of(g * GROUP, GROUP), GROUP)
        fields = advance(*loaded(now, below, above, at))
        for f in range(3):
            edge = 2 if f == 2 else 3
            for i in range(4):
                out[f, i, at, :] = fields[f][i]
                if i < edge:
                    first[3 * f + i, at, :] = fields[f][i].astype(bf16)
                if i >= 4 - edge:
                    last[3 * f + i - (4 - edge), at, :] = fields[f][i].astype(bf16)
        return carry

    lax.fori_loop(0, now.shape[2] // GROUP, group, 0)


def last_step_kernel(base, now, below, above, *refs):
    out = refs[-1]
    lane = lax.broadcasted_iota(jnp.int32, (GROUP, BLOCK), 1) < 64

    def group(g, carry):
        at = pl.ds(pl.multiple_of(g * GROUP, GROUP), GROUP)
        into = pl.ds(pl.multiple_of(base + g * GROUP, GROUP), GROUP)
        fields = advance(*loaded(now, below, above, at))
        for f in range(3):
            for p in range(2):
                to = p * HALF + f * BLOCK
                for t in range(4):
                    x = fields[f][2 * p][:, t * BLOCK : (t + 1) * BLOCK]
                    y = fields[f][2 * p + 1][:, t * BLOCK : (t + 1) * BLOCK]
                    even = jnp.where(lane, x, pltpu.roll(y, 64, 1))
                    odd = jnp.where(lane, pltpu.roll(x, 64, 1), y)
                    out[2 * t, into, to : to + BLOCK] = even.astype(bf16)
                    out[2 * t + 1, into, to : to + BLOCK] = odd.astype(bf16)
        return carry

    lax.fori_loop(0, now.shape[2] // GROUP, group, 0)


def swapped(last, first, up, down):
    return lax.ppermute(last, "space", up), lax.ppermute(first, "space", down)


def edges(fields):
    last = jnp.concatenate([fields[0, 1:], fields[1, 1:], fields[2, 2:]], axis=0)
    first = jnp.concatenate([fields[0, :3], fields[1, :3], fields[2, :2]], axis=0)
    return last, first


def step(kernel, outs, *arrays, aliases={}):
    return pl.pallas_call(
        kernel,
        out_shape=outs,
        in_specs=[vmem] * len(arrays),
        out_specs=jax.tree.map(lambda _: vmem, outs),
        input_output_aliases=aliases,
        compiler_params=pltpu.CompilerParams(vmem_limit_bytes=12 * 1024 * 1024),
        cost_estimate=pl.CostEstimate(
            flops=100_000_000 // PARTS, bytes_accessed=1_000_000, transcendentals=0
        ),
    )(*arrays)


def forecast(fields, up, down):
    _, rows, members, columns = fields.shape
    half = members // PARTS
    now_shape = jax.ShapeDtypeStruct((3, rows, half, columns), f32)
    edge_shape = jax.ShapeDtypeStruct((8, half, columns), bf16)
    chunk_shape = jax.ShapeDtypeStruct((columns // 64, members, COLS), bf16)
    parts = [fields[:, :, n * half : (n + 1) * half] for n in range(PARTS)]
    halos = [swapped(*edges(part), up, down) for part in parts]
    first_outs = (now_shape, edge_shape, edge_shape)
    chunks = ()
    for n in range(PARTS):
        now, first, last = step(first_step_kernel, first_outs, parts[n], *halos[n])
        halo = swapped(last, first, up, down)
        kernel = functools.partial(last_step_kernel, n * half)
        aliases = {3: 0} if chunks else {}
        chunks = (step(kernel, chunk_shape, now, *halo, *chunks, aliases=aliases),)
    return chunks[0]


def dot(a, b):
    return jnp.dot(a, b, preferred_element_type=f32)


def dot_t(a, b):
    return lax.dot_general(a, b, (((1,), (1,)), ((), ())), preferred_element_type=f32)


def split(a):
    high = a.astype(bf16)
    return high, (a - high.astype(f32)).astype(bf16)


def product(a, b):
    return dot(a[0], b[0]) + (dot(a[0], b[1]) + dot(a[1], b[0]))


def eye(n):
    return (
        lax.broadcasted_iota(jnp.int32, (n, n), 0) == lax.broadcasted_iota(jnp.int32, (n, n), 1)
    ).astype(f32)


def total(a):
    return jnp.sum(jnp.sum(a, axis=1, keepdims=True), axis=0, keepdims=True)


def weights_kernel(*refs):
    regions = refs[:HALVES]
    tile, index, value, var, packed, front, back = refs[HALVES : HALVES + 7]
    z_ref, zt_ref, b_ref, m_ref, l_ref, u_ref = refs[HALVES + 7 :]

    def put(start, rows):
        packed[start : start + rows.shape[0], :] = rows
        if start < FRONT:
            front[start : start + rows.shape[0], :] = rows
        else:
            back[start - FRONT : start - FRONT + rows.shape[0], :] = rows

    identity = eye(OBS)

    def as_column(row):
        return jnp.sum(identity * row, axis=1, keepdims=True)

    index_row = index[pl.ds(tile[0], 1), :]
    index_col = as_column(index_row.astype(f32)).astype(jnp.int32)
    var_row = var[...]
    var_col = as_column(var_row)
    own = jnp.concatenate(
        [
            jnp.concatenate([part[:, :BLOCK], part[:, HALF : HALF + BLOCK]], axis=1)
            for part in regions
        ],
        axis=0,
    )
    cell_row = lax.broadcasted_iota(jnp.int32, (CELLS, OBS), 0)
    pick = (cell_row == index_row).astype(f32).astype(bf16)
    cell_col = lax.broadcasted_iota(jnp.int32, (OBS, CELLS), 1)
    pick_t = (cell_col == index_col).astype(f32).astype(bf16)
    y = dot(own, pick)
    mean_row = jnp.sum(y, axis=0, keepdims=True) * (1.0 / MEMBERS)
    inverse_row = lax.rsqrt(var_row)
    z_ref[...] = (y - mean_row) * inverse_row
    y_t = dot_t(pick_t, own)
    mean_col = jnp.sum(y_t, axis=1, keepdims=True) * (1.0 / MEMBERS)
    zt_ref[...] = (y_t - mean_col) * lax.rsqrt(var_col)
    w_row = (value[...] - mean_row) * inverse_row

    b = product(split(zt_ref[...]), split(z_ref[...]))
    diagonal = float(MEMBERS - 1)
    squared = diagonal * diagonal * MEMBERS + 2.0 * diagonal * total(b * identity) + total(b * b)
    inverse_norm = lax.rsqrt(squared)
    alpha = diagonal * inverse_norm
    b = b * inverse_norm
    b_ref[...] = b

    low = 1.5 - 0.5 * alpha
    lower = low * identity - 0.5 * b
    l_ref[...] = lower
    u_ref[...] = alpha * lower + product(split(b), split(lower))
    m_ref[...] = -0.5 * identity

    def one_step(_, low):
        identity = eye(OBS)
        m = m_ref[...]
        lower = l_ref[...]
        l_parts = split(lower)
        u_parts = split(u_ref[...])
        step = split(1.5 * identity - 0.5 * product(l_parts, u_parts))
        part = split(-0.5 * (low * (alpha * m + lower) + product(split(m), u_parts)))
        factor = 1.5 - 0.5 * alpha * low * low
        l_ref[...] = product(step, l_parts)
        m_ref[...] = factor * m + product(part, l_parts)
        u_ref[...] = product(step, u_parts)
        return factor * low

    low = lax.fori_loop(0, NS_STEPS - 2, one_step, low)
    m = m_ref[...]
    lower = l_ref[...]
    part = -0.5 * (low * (alpha * m + lower) + product(split(m), split(u_ref[...])))
    factor = 1.5 - 0.5 * alpha * low * low
    m = factor * m + product(split(part), split(lower))
    low = factor * low

    b = b_ref[...]
    once = low * w_row + jnp.sum(
        m * jnp.sum(b * w_row, axis=1, keepdims=True), axis=0, keepdims=True
    )
    inner = jnp.sum(b * once, axis=1, keepdims=True)
    once_col = jnp.sum(identity * once, axis=1, keepdims=True)
    inner_row = jnp.sum(identity * inner, axis=0, keepdims=True)
    twice = low * once_col + jnp.sum(m * inner_row, axis=1, keepdims=True)
    centre = jnp.sum(zt_ref[...] * twice, axis=0, keepdims=True) * inverse_norm

    scale = math.sqrt(diagonal) * jnp.sqrt(inverse_norm)
    m_parts = split(m * (scale * inverse_norm))
    small = eye(BLOCK)
    spot = lax.broadcasted_iota(jnp.int32, (16, BLOCK), 0)
    at = 0
    for i in range(4):
        v = product(split(z_ref[i * BLOCK : (i + 1) * BLOCK, :]), m_parts)
        band = product(split(v), split(zt_ref[:, i * BLOCK :]))
        for j in range(i, 4):
            block = band[:, (j - i) * BLOCK : (j - i + 1) * BLOCK]
            if i == j:
                block = block + (scale * low) * small
            put(at, block.astype(bf16))
            at += BLOCK
        piece = centre[:, i * BLOCK : (i + 1) * BLOCK]
        high = piece.astype(bf16).astype(f32)
        both = jnp.where(spot == 0, high, jnp.where(spot == 1, piece - high, 0.0))
        put(CENTRE_AT + 16 * i, both.astype(bf16))


def region_weights(regions, tile, index, values, variances):
    return pl.pallas_call(
        weights_kernel,
        out_shape=[
            jax.ShapeDtypeStruct((size, BLOCK), bf16) for size in (PACKED, FRONT, PACKED - FRONT)
        ],
        in_specs=[vmem] * HALVES + [smem] + [vmem] * 3,
        out_specs=[vmem] * 3,
        scratch_shapes=[
            pltpu.VMEM((MEMBERS, OBS), f32),
            pltpu.VMEM((OBS, MEMBERS), f32),
            pltpu.VMEM((OBS, OBS), f32),
            pltpu.VMEM((OBS, OBS), f32),
            pltpu.VMEM((OBS, OBS), f32),
            pltpu.VMEM((OBS, OBS), f32),
        ],
        compiler_params=pltpu.CompilerParams(vmem_limit_bytes=24 * 1024 * 1024),
        cost_estimate=pl.CostEstimate(flops=6_000_000_000, bytes_accessed=1_000_000, transcendentals=0),
        name="weights",
    )(
        *regions,
        tile,
        index,
        values,
        variances,
    )


def column_parts(columns, parity):
    place = lax.broadcasted_iota(jnp.int32, (1, columns), 1)
    row = 2 * (place // HALF) + (place // 64) % 2
    col = place % 64
    row_weight = jnp.abs((row.astype(f32) + 0.5) / 4.0 - 0.5)
    col_weight = jnp.abs((col.astype(f32) + 0.5) / 64.0 - 0.5)
    right = (col >= 32).astype(jnp.int32)
    sibling = ((right + parity) == 1).astype(f32)
    return row_weight, col_weight, sibling


def factors(parity):
    r, q, sibling = column_parts(COLS, parity)
    side = {0: 1.0 - q, 1: q * sibling, 2: q * (1.0 - sibling)}
    return {(row, s): (r if row else 1.0 - r) * side[s] for row in (0, 1) for s in (0, 1, 2)}


def piece(source, start, size):
    if not isinstance(source, tuple):
        return source[start : start + size, :]
    if start < FRONT:
        return source[0][start : start + size, :]
    return source[1][start - FRONT : start - FRONT + size, :]


def unpack(source, full):
    for n, (i, j) in enumerate(PAIRS):
        block = piece(source, n * BLOCK, BLOCK)
        full[i * BLOCK : (i + 1) * BLOCK, j * BLOCK : (j + 1) * BLOCK] = block
        if i != j:
            turned = jnp.transpose(block)
            full[j * BLOCK : (j + 1) * BLOCK, i * BLOCK : (i + 1) * BLOCK] = turned


def apply(source, full, dev, acc, lo, hi, factor, before=None, out=None):
    unpack(source, full)
    for i in range(4):
        full[MEMBERS:, i * BLOCK : (i + 1) * BLOCK] = piece(source, CENTRE_AT + 16 * i, 16)

    def part(at):
        both = dot(full[...], dev[:, at])
        shift = jnp.sum(both[MEMBERS:], axis=0, keepdims=True)
        term = factor[:, at] * (both[:MEMBERS] + shift)
        term = term + (acc[:, at] if before is None else before[:, at])
        if out is None:
            acc[:, at] = term
        else:
            out[:, :, at] = term.astype(bf16).reshape(out.shape[0], out.shape[1], HALF)

    for at in range(lo, hi, HALF):
        part(slice(at, at + HALF))


def own_kernel(*refs):
    parity = refs[0]
    regions = refs[1 : 1 + HALVES]
    own, acc, dev, full, mean_ref = refs[1 + HALVES :]
    size = MEMBERS // HALVES
    for g in range(COLS // BLOCK):
        at = slice(g * BLOCK, (g + 1) * BLOCK)
        parts = [part[:, at].astype(f32) for part in regions]
        mean = sum(jnp.sum(part, axis=0, keepdims=True) for part in parts) * (1.0 / MEMBERS)
        mean_ref[:, at] = mean
        for n, part in enumerate(parts):
            dev[n * size : (n + 1) * size, at] = (part - mean).astype(bf16)
    apply(own, full, dev, acc, 0, COLS, factors(parity[0])[0, 0], before=mean_ref)


def near_kernel(
    parity, acc_in, dev, sibling, other_front, other_back, below, above, acc, full
):
    factor = factors(parity[0])
    apply(sibling, full, dev, acc, 0, COLS, factor[0, 1])
    apply((other_front, other_back), full, dev, acc, 0, COLS, factor[0, 2])
    apply(below, full, dev, acc, 0, HALF, factor[1, 0])
    apply(above, full, dev, acc, HALF, COLS, factor[1, 0])


def side_kernel(parity, acc_in, dev, below_sibling, above_sibling, acc, full):
    factor = factors(parity[0])
    apply(below_sibling, full, dev, acc, 0, HALF, factor[1, 1])
    apply(above_sibling, full, dev, acc, HALF, COLS, factor[1, 1])


def far_kernel(
    parity, acc, dev, below_front, below_back, above_front, above_back, out, full
):
    factor = factors(parity[0])
    apply((below_front, below_back), full, dev, acc, 0, HALF, factor[1, 2], out=out)
    apply((above_front, above_back), full, dev, acc, HALF, COLS, factor[1, 2], out=out)


def call(kernel, outs, flops, scratch, parity, *arrays, alias=False):
    return pl.pallas_call(
    kernel,
    out_shape=outs,
    in_specs=[smem] + [vmem] * len(arrays),
    out_specs=jax.tree.map(lambda _: vmem, outs),
    scratch_shapes=[pltpu.VMEM((MEMBERS + 16, MEMBERS), bf16)] + scratch,
    input_output_aliases={1: 0} if alias else {},
    compiler_params=pltpu.CompilerParams(vmem_limit_bytes=16 * 1024 * 1024),
    cost_estimate=pl.CostEstimate(flops=flops, bytes_accessed=1_000_000, transcendentals=0),
    )(parity, *arrays)


def restore_kernel(back, out, held):
    low = lax.broadcasted_iota(jnp.int32, (GROUP, BLOCK), 1) < 64

    def group(g, carry):
        at = pl.ds(pl.multiple_of(g * GROUP, GROUP), GROUP)
        for f in range(3):
            for p in range(2):
                place = p * HALF + f * BLOCK
                for t in range(4):
                    x = back[2 * t, at, place : place + BLOCK].astype(f32)
                    y = back[2 * t + 1, at, place : place + BLOCK].astype(f32)
                    first = jnp.where(low, x, pltpu.roll(y, 64, 1))
                    second = jnp.where(low, pltpu.roll(x, 64, 1), y)
                    held[t, pl.ds(2 * p, GROUP, stride=4), :] = first
                    held[t, pl.ds(2 * p + 1, GROUP, stride=4), :] = second
            for t in range(4):
                rows = held[t, :, :].reshape(GROUP, 4, BLOCK)
                out[0, at, f, :, t * BLOCK : (t + 1) * BLOCK] = rows.astype(bf16)
        return carry

    lax.fori_loop(0, back.shape[1] // GROUP, group, 0)


def restored(back):
    tiles, members, _ = back.shape
    columns = tiles * 64
    return pl.pallas_call(
        restore_kernel,
        out_shape=jax.ShapeDtypeStruct((1, members, 3, 4, columns), bf16),
        in_specs=[vmem],
        out_specs=vmem,
        scratch_shapes=[pltpu.VMEM((4, GROUP * 4, BLOCK), f32)],
        compiler_params=pltpu.CompilerParams(vmem_limit_bytes=12 * 1024 * 1024),
        cost_estimate=pl.CostEstimate(flops=10_000_000, bytes_accessed=1_000_000, transcendentals=0),
        name="restore",
    )(back)


def program(ensemble, obs_index, obs_value, obs_var):
    bands = lax.axis_size("space")
    tiles = lax.axis_size("member")
    tile = lax.axis_index("member")
    up = [(i, (i + 1) % bands) for i in range(bands)]
    down = [(j, i) for i, j in up]
    sibling_pairs = [(i, i ^ 1) for i in range(tiles)]
    other_pairs = [(i, (i + 1) % tiles if i % 2 else (i - 1) % tiles) for i in range(tiles)]

    near_members = ensemble.shape[1]
    fields, tile = lax.optimization_barrier((ensemble[0].transpose(1, 2, 0, 3), tile))
    parity = (tile % 2).astype(jnp.int32).reshape(1)
    chunks = forecast(fields, up, down)
    region = lax.all_to_all(chunks, "member", 0, 0, tiled=True).reshape(MEMBERS, COLS)
    regions = [region]
    own, front, behind = region_weights(regions, tile.reshape(1), obs_index[0, 0], obs_value[0, 0], obs_var[0, 0])

    other_front = lax.ppermute(front, "member", other_pairs)
    other_back = lax.ppermute(behind, "member", other_pairs)
    below = lax.ppermute(own, "space", up)
    above = lax.ppermute(own, "space", down)
    sibling = lax.ppermute(own, "member", sibling_pairs)
    below_front = lax.ppermute(other_front, "space", up)
    above_front = lax.ppermute(other_front, "space", down)
    below_back = lax.ppermute(other_back, "space", up)
    above_back = lax.ppermute(other_back, "space", down)
    below_sibling = lax.ppermute(below, "member", sibling_pairs)
    above_sibling = lax.ppermute(above, "member", sibling_pairs)
    total_shape = jax.ShapeDtypeStruct((MEMBERS, COLS), f32)
    dev_shape = jax.ShapeDtypeStruct((MEMBERS, COLS), bf16)
    out_shape = jax.ShapeDtypeStruct((tiles, near_members, COLS), bf16)
    mean_scratch = [pltpu.VMEM((1, COLS), f32)]
    acc, dev = call(own_kernel, (total_shape, dev_shape), 400_000_000, mean_scratch, parity, *regions, own)
    acc = call(near_kernel, total_shape, 1_200_000_000, [], parity, acc, dev, sibling, other_front, other_back, below, above, alias=True)
    acc = call(side_kernel, total_shape, 400_000_000, [], parity, acc, dev, below_sibling, above_sibling, alias=True)
    analysed = call(far_kernel, out_shape, 400_000_000, [], parity, acc, dev, below_front, below_back, above_front, above_back)
    back = lax.all_to_all(analysed, "member", 0, 0, tiled=True)
    return restored(back)


def solution(mesh):
    return jax.shard_map(
        program,
        mesh=mesh,
        in_specs=(
            P("group", "member", None, "space", None),
            P("group", "space", None, None),
            P("group", "space", "member", None),
            P("group", "space", "member", None),
        ),
        out_specs=P("group", "member", None, "space", None),
        check_vma=False,
    )
```

```python
import functools
import math

import jax
import jax.numpy as jnp
from jax import lax
from jax.experimental import pallas as pl
from jax.experimental.pallas import tpu as pltpu
from jax.sharding import PartitionSpec as P

NS_STEPS = 6
MEMBERS = 512
CELLS = 256
OBS = 256
BLOCK = 128
PAIRS = [(i, j) for i in range(4) for j in range(i, 4)]
CENTRE_AT = len(PAIRS) * BLOCK
PACKED = CENTRE_AT + 16

time_step = 0.4
coriolis = 0.3
COLS = 768
HALF = 384
HALVES = 1
PARTS = 2
f32 = jnp.float32
bf16 = jnp.bfloat16
vmem = pl.BlockSpec(memory_space=pltpu.VMEM)
smem = pl.BlockSpec(memory_space=pltpu.SMEM)


def column_difference(field):
    columns = field.shape[-1]
    return 0.5 * (pltpu.roll(field, columns - 1, 1) - pltpu.roll(field, 1, 1))


def rates(h, v, u, i):
    d_height = -(column_difference(u[i]) + 0.5 * (v[i + 1] - v[i - 1]))
    d_north = -0.5 * (h[i + 1] - h[i - 1]) - coriolis * u[i]
    return d_height, d_north


def rate_east(h, v, i):
    return coriolis * v[i] - column_difference(h[i])


def advance(h0, v0, u0):
    h1, v1, u1, h2, v2, u2, h3, v3, u3 = ({} for _ in range(9))
    for i in range(-2, 6):
        dh, dv = rates(h0, v0, u0, i)
        h1[i] = h0[i] + time_step * dh
        v1[i] = v0[i] + time_step * dv
        if -1 <= i <= 4:
            u1[i] = u0[i] + time_step * rate_east(h0, v0, i)
    for i in range(-1, 5):
        dh, dv = rates(h1, v1, u1, i)
        h2[i] = 0.75 * h0[i] + 0.25 * (h1[i] + time_step * dh)
        v2[i] = 0.75 * v0[i] + 0.25 * (v1[i] + time_step * dv)
        if 0 <= i <= 3:
            u2[i] = 0.75 * u0[i] + 0.25 * (u1[i] + time_step * rate_east(h1, v1, i))
    third = 1.0 / 3.0
    two_thirds = 2.0 / 3.0
    for i in range(4):
        dh, dv = rates(h2, v2, u2, i)
        h3[i] = h0[i] * third + two_thirds * (h2[i] + time_step * dh)
        v3[i] = v0[i] * third + two_thirds * (v2[i] + time_step * dv)
        u3[i] = u0[i] * third + two_thirds * (u2[i] + time_step * rate_east(h2, v2, i))
    return h3, v3, u3


GROUP = 16


def loaded(now, below, above, at):
    h, v, u = {}, {}, {}
    for f, field in enumerate((h, v, u)):
        for i in range(4):
            field[i] = now[f, i, at, :].astype(f32)
    for k in range(3):
        h[k - 3] = below[k, at, :].astype(f32)
        v[k - 3] = below[3 + k, at, :].astype(f32)
        h[4 + k] = above[k, at, :].astype(f32)
        v[4 + k] = above[3 + k, at, :].astype(f32)
    for k in range(2):
        u[k - 2] = below[6 + k, at, :].astype(f32)
        u[4 + k] = above[6 + k, at, :].astype(f32)
    return h, v, u


def first_step_kernel(now, below, above, out, first, last):
    def group(g, carry):
        at = pl.ds(pl.multiple_of(g * GROUP, GROUP), GROUP)
        fields = advance(*loaded(now, below, above, at))
        for f in range(3):
            edge = 2 if f == 2 else 3
            for i in range(4):
                out[f, i, at, :] = fields[f][i]
                if i < edge:
                    first[3 * f + i, at, :] = fields[f][i].astype(bf16)
                if i >= 4 - edge:
                    last[3 * f + i - (4 - edge), at, :] = fields[f][i].astype(bf16)
        return carry

    lax.fori_loop(0, now.shape[2] // GROUP, group, 0)


def last_step_kernel(base, now, below, above, *refs):
    out = refs[-1]
    lane = lax.broadcasted_iota(jnp.int32, (GROUP, BLOCK), 1) < 64

    def group(g, carry):
        at = pl.ds(pl.multiple_of(g * GROUP, GROUP), GROUP)
        into = pl.ds(pl.multiple_of(base + g * GROUP, GROUP), GROUP)
        fields = advance(*loaded(now, below, above, at))
        for f in range(3):
            for p in range(2):
                to = p * HALF + f * BLOCK
                for t in range(4):
                    x = fields[f][2 * p][:, t * BLOCK : (t + 1) * BLOCK]
                    y = fields[f][2 * p + 1][:, t * BLOCK : (t + 1) * BLOCK]
                    even = jnp.where(lane, x, pltpu.roll(y, 64, 1))
                    odd = jnp.where(lane, pltpu.roll(x, 64, 1), y)
                    out[2 * t, into, to : to + BLOCK] = even.astype(bf16)
                    out[2 * t + 1, into, to : to + BLOCK] = odd.astype(bf16)
        return carry

    lax.fori_loop(0, now.shape[2] // GROUP, group, 0)


def swapped(last, first, up, down):
    return lax.ppermute(last, "space", up), lax.ppermute(first, "space", down)


def edges(fields):
    last = jnp.concatenate([fields[0, 1:], fields[1, 1:], fields[2, 2:]], axis=0)
    first = jnp.concatenate([fields[0, :3], fields[1, :3], fields[2, :2]], axis=0)
    return last, first


def step(kernel, outs, *arrays, aliases={}):
    return pl.pallas_call(
        kernel,
        out_shape=outs,
        in_specs=[vmem] * len(arrays),
        out_specs=jax.tree.map(lambda _: vmem, outs),
        input_output_aliases=aliases,
        compiler_params=pltpu.CompilerParams(vmem_limit_bytes=12 * 1024 * 1024),
        cost_estimate=pl.CostEstimate(
            flops=100_000_000 // PARTS, bytes_accessed=1_000_000, transcendentals=0
        ),
    )(*arrays)


def forecast(fields, up, down):
    _, rows, members, columns = fields.shape
    half = members // PARTS
    now_shape = jax.ShapeDtypeStruct((3, rows, half, columns), f32)
    edge_shape = jax.ShapeDtypeStruct((8, half, columns), bf16)
    chunk_shape = jax.ShapeDtypeStruct((columns // 64, members, COLS), bf16)
    parts = [fields[:, :, n * half : (n + 1) * half] for n in range(PARTS)]
    halos = [swapped(*edges(part), up, down) for part in parts]
    first_outs = (now_shape, edge_shape, edge_shape)
    chunks = ()
    for n in range(PARTS):
        now, first, last = step(first_step_kernel, first_outs, parts[n], *halos[n])
        halo = swapped(last, first, up, down)
        kernel = functools.partial(last_step_kernel, n * half)
        aliases = {3: 0} if chunks else {}
        chunks = (step(kernel, chunk_shape, now, *halo, *chunks, aliases=aliases),)
    return chunks[0]


def dot(a, b):
    return jnp.dot(a, b, preferred_element_type=f32)


def dot_t(a, b):
    return lax.dot_general(a, b, (((1,), (1,)), ((), ())), preferred_element_type=f32)


def split(a):
    high = a.astype(bf16)
    return high, (a - high.astype(f32)).astype(bf16)


def product(a, b):
    return dot(a[0], b[0]) + (dot(a[0], b[1]) + dot(a[1], b[0]))


def eye(n):
    return (
        lax.broadcasted_iota(jnp.int32, (n, n), 0) == lax.broadcasted_iota(jnp.int32, (n, n), 1)
    ).astype(f32)


def total(a):
    return jnp.sum(jnp.sum(a, axis=1, keepdims=True), axis=0, keepdims=True)


def weights_kernel(*refs):
    regions = refs[:HALVES]
    tile, index, value, var, packed = refs[HALVES : HALVES + 5]
    z_ref, zt_ref, b_ref, m_ref, l_ref, u_ref = refs[HALVES + 5 :]
    identity = eye(OBS)

    def as_column(row):
        return jnp.sum(identity * row, axis=1, keepdims=True)

    index_row = index[pl.ds(tile[0], 1), :]
    index_col = as_column(index_row.astype(f32)).astype(jnp.int32)
    var_row = var[...]
    var_col = as_column(var_row)
    own = jnp.concatenate(
        [
            jnp.concatenate([part[:, :BLOCK], part[:, HALF : HALF + BLOCK]], axis=1)
            for part in regions
        ],
        axis=0,
    )
    cell_row = lax.broadcasted_iota(jnp.int32, (CELLS, OBS), 0)
    pick = (cell_row == index_row).astype(f32).astype(bf16)
    cell_col = lax.broadcasted_iota(jnp.int32, (OBS, CELLS), 1)
    pick_t = (cell_col == index_col).astype(f32).astype(bf16)
    y = dot(own, pick)
    mean_row = jnp.sum(y, axis=0, keepdims=True) * (1.0 / MEMBERS)
    inverse_row = lax.rsqrt(var_row)
    z_ref[...] = (y - mean_row) * inverse_row
    y_t = dot_t(pick_t, own)
    mean_col = jnp.sum(y_t, axis=1, keepdims=True) * (1.0 / MEMBERS)
    zt_ref[...] = (y_t - mean_col) * lax.rsqrt(var_col)
    w_row = (value[...] - mean_row) * inverse_row

    b = product(split(zt_ref[...]), split(z_ref[...]))
    diagonal = float(MEMBERS - 1)
    squared = diagonal * diagonal * MEMBERS + 2.0 * diagonal * total(b * identity) + total(b * b)
    inverse_norm = lax.rsqrt(squared)
    alpha = diagonal * inverse_norm
    b = b * inverse_norm
    b_ref[...] = b

    low = 1.5 - 0.5 * alpha
    lower = low * identity - 0.5 * b
    l_ref[...] = lower
    u_ref[...] = alpha * lower + product(split(b), split(lower))
    m_ref[...] = -0.5 * identity

    def one_step(_, low):
        identity = eye(OBS)
        m = m_ref[...]
        lower = l_ref[...]
        l_parts = split(lower)
        u_parts = split(u_ref[...])
        step = split(1.5 * identity - 0.5 * product(l_parts, u_parts))
        part = split(-0.5 * (low * (alpha * m + lower) + product(split(m), u_parts)))
        factor = 1.5 - 0.5 * alpha * low * low
        l_ref[...] = product(step, l_parts)
        m_ref[...] = factor * m + product(part, l_parts)
        u_ref[...] = product(step, u_parts)
        return factor * low

    low = lax.fori_loop(0, NS_STEPS - 2, one_step, low)
    m = m_ref[...]
    lower = l_ref[...]
    part = -0.5 * (low * (alpha * m + lower) + product(split(m), split(u_ref[...])))
    factor = 1.5 - 0.5 * alpha * low * low
    m = factor * m + product(split(part), split(lower))
    low = factor * low

    b = b_ref[...]
    once = low * w_row + jnp.sum(
        m * jnp.sum(b * w_row, axis=1, keepdims=True), axis=0, keepdims=True
    )
    inner = jnp.sum(b * once, axis=1, keepdims=True)
    once_col = jnp.sum(identity * once, axis=1, keepdims=True)
    inner_row = jnp.sum(identity * inner, axis=0, keepdims=True)
    twice = low * once_col + jnp.sum(m * inner_row, axis=1, keepdims=True)
    centre = jnp.sum(zt_ref[...] * twice, axis=0, keepdims=True) * inverse_norm

    scale = math.sqrt(diagonal) * jnp.sqrt(inverse_norm)
    m_parts = split(m * (scale * inverse_norm))
    small = eye(BLOCK)
    spot = lax.broadcasted_iota(jnp.int32, (16, BLOCK), 0)
    both = jnp.zeros((16, BLOCK), f32)
    at = 0
    for i in range(4):
        v = product(split(z_ref[i * BLOCK : (i + 1) * BLOCK, :]), m_parts)
        band = product(split(v), split(zt_ref[:, i * BLOCK :]))
        for j in range(i, 4):
            block = band[:, (j - i) * BLOCK : (j - i + 1) * BLOCK]
            if i == j:
                block = block + (scale * low) * small
            packed[at : at + BLOCK, :] = block.astype(bf16)
            at += BLOCK
        along = centre[:, i * BLOCK : (i + 1) * BLOCK]
        high = along.astype(bf16).astype(f32)
        both = both + jnp.where(spot == i, high, jnp.where(spot == 4 + i, along - high, 0.0))
    packed[CENTRE_AT:, :] = both.astype(bf16)


def region_weights(regions, tile, index, values, variances):
    return pl.pallas_call(
        weights_kernel,
        out_shape=jax.ShapeDtypeStruct((PACKED, BLOCK), bf16),
        in_specs=[vmem] * HALVES + [smem] + [vmem] * 3,
        out_specs=vmem,
        scratch_shapes=[
            pltpu.VMEM((MEMBERS, OBS), f32),
            pltpu.VMEM((OBS, MEMBERS), f32),
            pltpu.VMEM((OBS, OBS), f32),
            pltpu.VMEM((OBS, OBS), f32),
            pltpu.VMEM((OBS, OBS), f32),
            pltpu.VMEM((OBS, OBS), f32),
        ],
        compiler_params=pltpu.CompilerParams(vmem_limit_bytes=24 * 1024 * 1024),
        cost_estimate=pl.CostEstimate(flops=6_000_000_000, bytes_accessed=1_000_000, transcendentals=0),
        name="weights",
    )(
        *regions,
        tile,
        index,
        values,
        variances,
    )


def column_parts(columns, parity):
    place = lax.broadcasted_iota(jnp.int32, (1, columns), 1)
    row = 2 * (place // HALF) + (place // 64) % 2
    col = place % 64
    row_weight = jnp.abs((row.astype(f32) + 0.5) / 4.0 - 0.5)
    col_weight = jnp.abs((col.astype(f32) + 0.5) / 64.0 - 0.5)
    right = (col >= 32).astype(jnp.int32)
    sibling = ((right + parity) == 1).astype(f32)
    return row_weight, col_weight, sibling


def factors(parity):
    r, q, sibling = column_parts(COLS, parity)
    side = {0: 1.0 - q, 1: q * sibling, 2: q * (1.0 - sibling)}
    return {(row, s): (r if row else 1.0 - r) * side[s] for row in (0, 1) for s in (0, 1, 2)}


def unpack(source, full):
    for n, (i, j) in enumerate(PAIRS):
        block = source[n * BLOCK : (n + 1) * BLOCK, :]
        full[i * BLOCK : (i + 1) * BLOCK, j * BLOCK : (j + 1) * BLOCK] = block
        if i != j:
            turned = jnp.transpose(block)
            full[j * BLOCK : (j + 1) * BLOCK, i * BLOCK : (i + 1) * BLOCK] = turned


def apply(source, full, dev, acc, lo, hi, factor, before=None, out=None):
    unpack(source, full)
    spot = lax.broadcasted_iota(jnp.int32, (16, BLOCK), 0)
    centre = source[CENTRE_AT:, :].astype(f32)
    for i in range(4):
        mine = jnp.where(spot % 4 == i, centre, 0.0)
        full[MEMBERS:, i * BLOCK : (i + 1) * BLOCK] = mine.astype(bf16)

    def part(at):
        both = dot(full[...], dev[:, at])
        shift = jnp.sum(both[MEMBERS:], axis=0, keepdims=True)
        term = factor[:, at] * (both[:MEMBERS] + shift)
        term = term + (acc[:, at] if before is None else before[:, at])
        if out is None:
            acc[:, at] = term
        else:
            out[:, :, at] = term.astype(bf16).reshape(out.shape[0], out.shape[1], HALF)

    for at in range(lo, hi, HALF):
        part(slice(at, at + HALF))


def own_kernel(*refs):
    parity = refs[0]
    regions = refs[1 : 1 + HALVES]
    own, acc, dev, full, mean_ref = refs[1 + HALVES :]
    size = MEMBERS // HALVES
    for g in range(COLS // BLOCK):
        at = slice(g * BLOCK, (g + 1) * BLOCK)
        parts = [part[:, at].astype(f32) for part in regions]
        mean = sum(jnp.sum(part, axis=0, keepdims=True) for part in parts) * (1.0 / MEMBERS)
        mean_ref[:, at] = mean
        for n, part in enumerate(parts):
            dev[n * size : (n + 1) * size, at] = (part - mean).astype(bf16)
    apply(own, full, dev, acc, 0, COLS, factors(parity[0])[0, 0], before=mean_ref)


def near_kernel(
    parity, acc_in, dev, sibling, other, below, above, acc, full
):
    factor = factors(parity[0])
    apply(sibling, full, dev, acc, 0, COLS, factor[0, 1])
    apply(other, full, dev, acc, 0, COLS, factor[0, 2])
    apply(below, full, dev, acc, 0, HALF, factor[1, 0])
    apply(above, full, dev, acc, HALF, COLS, factor[1, 0])


def side_kernel(parity, acc_in, dev, below_sibling, above_sibling, acc, full):
    factor = factors(parity[0])
    apply(below_sibling, full, dev, acc, 0, HALF, factor[1, 1])
    apply(above_sibling, full, dev, acc, HALF, COLS, factor[1, 1])


def far_kernel(
    parity, acc, dev, below_other, above_other, out, full
):
    factor = factors(parity[0])
    apply(below_other, full, dev, acc, 0, HALF, factor[1, 2], out=out)
    apply(above_other, full, dev, acc, HALF, COLS, factor[1, 2], out=out)


def call(kernel, outs, flops, scratch, parity, *arrays, alias=False):
    return pl.pallas_call(
    kernel,
    out_shape=outs,
    in_specs=[smem] + [vmem] * len(arrays),
    out_specs=jax.tree.map(lambda _: vmem, outs),
    scratch_shapes=[pltpu.VMEM((MEMBERS + 16, MEMBERS), bf16)] + scratch,
    input_output_aliases={1: 0} if alias else {},
    compiler_params=pltpu.CompilerParams(vmem_limit_bytes=16 * 1024 * 1024),
    cost_estimate=pl.CostEstimate(flops=flops, bytes_accessed=1_000_000, transcendentals=0),
    )(parity, *arrays)


def restore_kernel(back, out, held):
    low = lax.broadcasted_iota(jnp.int32, (GROUP, BLOCK), 1) < 64

    def group(g, carry):
        at = pl.ds(pl.multiple_of(g * GROUP, GROUP), GROUP)
        for f in range(3):
            for p in range(2):
                place = p * HALF + f * BLOCK
                for t in range(4):
                    x = back[2 * t, at, place : place + BLOCK].astype(f32)
                    y = back[2 * t + 1, at, place : place + BLOCK].astype(f32)
                    first = jnp.where(low, x, pltpu.roll(y, 64, 1))
                    second = jnp.where(low, pltpu.roll(x, 64, 1), y)
                    held[t, pl.ds(2 * p, GROUP, stride=4), :] = first
                    held[t, pl.ds(2 * p + 1, GROUP, stride=4), :] = second
            for t in range(4):
                rows = held[t, :, :].reshape(GROUP, 4, BLOCK)
                out[0, at, f, :, t * BLOCK : (t + 1) * BLOCK] = rows.astype(bf16)
        return carry

    lax.fori_loop(0, back.shape[1] // GROUP, group, 0)


def restored(back):
    tiles, members, _ = back.shape
    columns = tiles * 64
    return pl.pallas_call(
        restore_kernel,
        out_shape=jax.ShapeDtypeStruct((1, members, 3, 4, columns), bf16),
        in_specs=[vmem],
        out_specs=vmem,
        scratch_shapes=[pltpu.VMEM((4, GROUP * 4, BLOCK), f32)],
        compiler_params=pltpu.CompilerParams(vmem_limit_bytes=12 * 1024 * 1024),
        cost_estimate=pl.CostEstimate(flops=10_000_000, bytes_accessed=1_000_000, transcendentals=0),
        name="restore",
    )(back)


def program(ensemble, obs_index, obs_value, obs_var):
    bands = lax.axis_size("space")
    tiles = lax.axis_size("member")
    tile = lax.axis_index("member")
    up = [(i, (i + 1) % bands) for i in range(bands)]
    down = [(j, i) for i, j in up]
    sibling_pairs = [(i, i ^ 1) for i in range(tiles)]
    other_pairs = [(i, (i + 1) % tiles if i % 2 else (i - 1) % tiles) for i in range(tiles)]

    near_members = ensemble.shape[1]
    fields, tile = lax.optimization_barrier((ensemble[0].transpose(1, 2, 0, 3), tile))
    parity = (tile % 2).astype(jnp.int32).reshape(1)
    chunks = forecast(fields, up, down)
    region = lax.all_to_all(chunks, "member", 0, 0, tiled=True).reshape(MEMBERS, COLS)
    regions = [region]
    own = region_weights(regions, tile.reshape(1), obs_index[0, 0], obs_value[0, 0], obs_var[0, 0])

    other = lax.ppermute(own, "member", other_pairs)
    below = lax.ppermute(own, "space", up)
    above = lax.ppermute(own, "space", down)
    sibling = lax.ppermute(own, "member", sibling_pairs)
    below_other = lax.ppermute(other, "space", up)
    above_other = lax.ppermute(other, "space", down)
    below_sibling = lax.ppermute(below, "member", sibling_pairs)
    above_sibling = lax.ppermute(above, "member", sibling_pairs)
    total_shape = jax.ShapeDtypeStruct((MEMBERS, COLS), f32)
    dev_shape = jax.ShapeDtypeStruct((MEMBERS, COLS), bf16)
    out_shape = jax.ShapeDtypeStruct((tiles, near_members, COLS), bf16)
    mean_scratch = [pltpu.VMEM((1, COLS), f32)]
    acc, dev = call(own_kernel, (total_shape, dev_shape), 400_000_000, mean_scratch, parity, *regions, own)
    acc = call(near_kernel, total_shape, 1_200_000_000, [], parity, acc, dev, sibling, other, below, above, alias=True)
    acc = call(side_kernel, total_shape, 400_000_000, [], parity, acc, dev, below_sibling, above_sibling, alias=True)
    analysed = call(far_kernel, out_shape, 400_000_000, [], parity, acc, dev, below_other, above_other)
    back = lax.all_to_all(analysed, "member", 0, 0, tiled=True)
    return restored(back)


def solution(mesh):
    return jax.shard_map(
        program,
        mesh=mesh,
        in_specs=(
            P("group", "member", None, "space", None),
            P("group", "space", None, None),
            P("group", "space", "member", None),
            P("group", "space", "member", None),
        ),
        out_specs=P("group", "member", None, "space", None),
        check_vma=False,
    )
```

```python
import functools
import math

import jax
import jax.numpy as jnp
from jax import lax
from jax.experimental import pallas as pl
from jax.experimental.pallas import tpu as pltpu
from jax.sharding import PartitionSpec as P

NS_STEPS = 6
MEMBERS = 512
CELLS = 256
OBS = 256
BLOCK = 128
PAIRS = [(i, j) for i in range(4) for j in range(i, 4)]
SPOTS = {pair: n * BLOCK for n, pair in enumerate(PAIRS)}
CENTRE_AT = SPOTS[3, 3]
PACKED = CENTRE_AT + 16

time_step = 0.4
coriolis = 0.3
COLS = 768
HALF = 384
HALVES = 1
PARTS = 2
f32 = jnp.float32
bf16 = jnp.bfloat16
vmem = pl.BlockSpec(memory_space=pltpu.VMEM)
smem = pl.BlockSpec(memory_space=pltpu.SMEM)


def column_difference(field):
    columns = field.shape[-1]
    return 0.5 * (pltpu.roll(field, columns - 1, 1) - pltpu.roll(field, 1, 1))


def rates(h, v, u, i):
    d_height = -(column_difference(u[i]) + 0.5 * (v[i + 1] - v[i - 1]))
    d_north = -0.5 * (h[i + 1] - h[i - 1]) - coriolis * u[i]
    return d_height, d_north


def rate_east(h, v, i):
    return coriolis * v[i] - column_difference(h[i])


def advance(h0, v0, u0):
    h1, v1, u1, h2, v2, u2, h3, v3, u3 = ({} for _ in range(9))
    for i in range(-2, 6):
        dh, dv = rates(h0, v0, u0, i)
        h1[i] = h0[i] + time_step * dh
        v1[i] = v0[i] + time_step * dv
        if -1 <= i <= 4:
            u1[i] = u0[i] + time_step * rate_east(h0, v0, i)
    for i in range(-1, 5):
        dh, dv = rates(h1, v1, u1, i)
        h2[i] = 0.75 * h0[i] + 0.25 * (h1[i] + time_step * dh)
        v2[i] = 0.75 * v0[i] + 0.25 * (v1[i] + time_step * dv)
        if 0 <= i <= 3:
            u2[i] = 0.75 * u0[i] + 0.25 * (u1[i] + time_step * rate_east(h1, v1, i))
    third = 1.0 / 3.0
    two_thirds = 2.0 / 3.0
    for i in range(4):
        dh, dv = rates(h2, v2, u2, i)
        h3[i] = h0[i] * third + two_thirds * (h2[i] + time_step * dh)
        v3[i] = v0[i] * third + two_thirds * (v2[i] + time_step * dv)
        u3[i] = u0[i] * third + two_thirds * (u2[i] + time_step * rate_east(h2, v2, i))
    return h3, v3, u3


GROUP = 16


def loaded(now, below, above, at):
    h, v, u = {}, {}, {}
    for f, field in enumerate((h, v, u)):
        for i in range(4):
            field[i] = now[f, i, at, :].astype(f32)
    for k in range(3):
        h[k - 3] = below[k, at, :].astype(f32)
        v[k - 3] = below[3 + k, at, :].astype(f32)
        h[4 + k] = above[k, at, :].astype(f32)
        v[4 + k] = above[3 + k, at, :].astype(f32)
    for k in range(2):
        u[k - 2] = below[6 + k, at, :].astype(f32)
        u[4 + k] = above[6 + k, at, :].astype(f32)
    return h, v, u


def first_step_kernel(now, below, above, out, first, last):
    def group(g, carry):
        at = pl.ds(pl.multiple_of(g * GROUP, GROUP), GROUP)
        fields = advance(*loaded(now, below, above, at))
        for f in range(3):
            edge = 2 if f == 2 else 3
            for i in range(4):
                out[f, i, at, :] = fields[f][i]
                if i < edge:
                    first[3 * f + i, at, :] = fields[f][i].astype(bf16)
                if i >= 4 - edge:
                    last[3 * f + i - (4 - edge), at, :] = fields[f][i].astype(bf16)
        return carry

    lax.fori_loop(0, now.shape[2] // GROUP, group, 0)


def last_step_kernel(base, now, below, above, *refs):
    out = refs[-1]
    lane = lax.broadcasted_iota(jnp.int32, (GROUP, BLOCK), 1) < 64

    def group(g, carry):
        at = pl.ds(pl.multiple_of(g * GROUP, GROUP), GROUP)
        into = pl.ds(pl.multiple_of(base + g * GROUP, GROUP), GROUP)
        fields = advance(*loaded(now, below, above, at))
        for f in range(3):
            for p in range(2):
                to = p * HALF + f * BLOCK
                for t in range(4):
                    x = fields[f][2 * p][:, t * BLOCK : (t + 1) * BLOCK]
                    y = fields[f][2 * p + 1][:, t * BLOCK : (t + 1) * BLOCK]
                    even = jnp.where(lane, x, pltpu.roll(y, 64, 1))
                    odd = jnp.where(lane, pltpu.roll(x, 64, 1), y)
                    out[2 * t, into, to : to + BLOCK] = even.astype(bf16)
                    out[2 * t + 1, into, to : to + BLOCK] = odd.astype(bf16)
        return carry

    lax.fori_loop(0, now.shape[2] // GROUP, group, 0)


def swapped(last, first, up, down):
    return lax.ppermute(last, "space", up), lax.ppermute(first, "space", down)


def edges(fields):
    last = jnp.concatenate([fields[0, 1:], fields[1, 1:], fields[2, 2:]], axis=0)
    first = jnp.concatenate([fields[0, :3], fields[1, :3], fields[2, :2]], axis=0)
    return last, first


def step(kernel, outs, *arrays, aliases={}):
    return pl.pallas_call(
        kernel,
        out_shape=outs,
        in_specs=[vmem] * len(arrays),
        out_specs=jax.tree.map(lambda _: vmem, outs),
        input_output_aliases=aliases,
        compiler_params=pltpu.CompilerParams(vmem_limit_bytes=12 * 1024 * 1024),
        cost_estimate=pl.CostEstimate(
            flops=100_000_000 // PARTS, bytes_accessed=1_000_000, transcendentals=0
        ),
    )(*arrays)


def forecast(fields, up, down):
    _, rows, members, columns = fields.shape
    half = members // PARTS
    now_shape = jax.ShapeDtypeStruct((3, rows, half, columns), f32)
    edge_shape = jax.ShapeDtypeStruct((8, half, columns), bf16)
    chunk_shape = jax.ShapeDtypeStruct((columns // 64, members, COLS), bf16)
    parts = [fields[:, :, n * half : (n + 1) * half] for n in range(PARTS)]
    halos = [swapped(*edges(part), up, down) for part in parts]
    first_outs = (now_shape, edge_shape, edge_shape)
    chunks = ()
    for n in range(PARTS):
        now, first, last = step(first_step_kernel, first_outs, parts[n], *halos[n])
        halo = swapped(last, first, up, down)
        kernel = functools.partial(last_step_kernel, n * half)
        aliases = {3: 0} if chunks else {}
        chunks = (step(kernel, chunk_shape, now, *halo, *chunks, aliases=aliases),)
    return chunks[0]


def dot(a, b):
    return jnp.dot(a, b, preferred_element_type=f32)


def dot_t(a, b):
    return lax.dot_general(a, b, (((1,), (1,)), ((), ())), preferred_element_type=f32)


def split(a):
    high = a.astype(bf16)
    return high, (a - high.astype(f32)).astype(bf16)


def product(a, b):
    return dot(a[0], b[0]) + (dot(a[0], b[1]) + dot(a[1], b[0]))


def eye(n):
    return (
        lax.broadcasted_iota(jnp.int32, (n, n), 0) == lax.broadcasted_iota(jnp.int32, (n, n), 1)
    ).astype(f32)


def total(a):
    return jnp.sum(jnp.sum(a, axis=1, keepdims=True), axis=0, keepdims=True)


def weights_kernel(*refs):
    regions = refs[:HALVES]
    tile, index, value, var, packed = refs[HALVES : HALVES + 5]
    z_ref, zt_ref, b_ref, m_ref, l_ref, u_ref = refs[HALVES + 5 :]
    identity = eye(OBS)

    def as_column(row):
        return jnp.sum(identity * row, axis=1, keepdims=True)

    index_row = index[pl.ds(tile[0], 1), :]
    index_col = as_column(index_row.astype(f32)).astype(jnp.int32)
    var_row = var[...]
    var_col = as_column(var_row)
    own = jnp.concatenate(
        [
            jnp.concatenate([part[:, :BLOCK], part[:, HALF : HALF + BLOCK]], axis=1)
            for part in regions
        ],
        axis=0,
    )
    cell_row = lax.broadcasted_iota(jnp.int32, (CELLS, OBS), 0)
    pick = (cell_row == index_row).astype(f32).astype(bf16)
    cell_col = lax.broadcasted_iota(jnp.int32, (OBS, CELLS), 1)
    pick_t = (cell_col == index_col).astype(f32).astype(bf16)
    y = dot(own, pick)
    mean_row = jnp.sum(y, axis=0, keepdims=True) * (1.0 / MEMBERS)
    inverse_row = lax.rsqrt(var_row)
    z_ref[...] = (y - mean_row) * inverse_row
    y_t = dot_t(pick_t, own)
    mean_col = jnp.sum(y_t, axis=1, keepdims=True) * (1.0 / MEMBERS)
    zt_ref[...] = (y_t - mean_col) * lax.rsqrt(var_col)
    w_row = (value[...] - mean_row) * inverse_row

    b = product(split(zt_ref[...]), split(z_ref[...]))
    diagonal = float(MEMBERS - 1)
    squared = diagonal * diagonal * MEMBERS + 2.0 * diagonal * total(b * identity) + total(b * b)
    inverse_norm = lax.rsqrt(squared)
    alpha = diagonal * inverse_norm
    b = b * inverse_norm
    b_ref[...] = b

    low = 1.5 - 0.5 * alpha
    lower = low * identity - 0.5 * b
    l_ref[...] = lower
    u_ref[...] = alpha * lower + product(split(b), split(lower))
    m_ref[...] = -0.5 * identity

    def one_step(_, low):
        identity = eye(OBS)
        m = m_ref[...]
        lower = l_ref[...]
        l_parts = split(lower)
        u_parts = split(u_ref[...])
        step = split(1.5 * identity - 0.5 * product(l_parts, u_parts))
        part = split(-0.5 * (low * (alpha * m + lower) + product(split(m), u_parts)))
        factor = 1.5 - 0.5 * alpha * low * low
        l_ref[...] = product(step, l_parts)
        m_ref[...] = factor * m + product(part, l_parts)
        u_ref[...] = product(step, u_parts)
        return factor * low

    low = lax.fori_loop(0, NS_STEPS - 2, one_step, low)
    m = m_ref[...]
    lower = l_ref[...]
    part = -0.5 * (low * (alpha * m + lower) + product(split(m), split(u_ref[...])))
    factor = 1.5 - 0.5 * alpha * low * low
    m = factor * m + product(split(part), split(lower))
    low = factor * low

    b = b_ref[...]
    once = low * w_row + jnp.sum(
        m * jnp.sum(b * w_row, axis=1, keepdims=True), axis=0, keepdims=True
    )
    inner = jnp.sum(b * once, axis=1, keepdims=True)
    once_col = jnp.sum(identity * once, axis=1, keepdims=True)
    inner_row = jnp.sum(identity * inner, axis=0, keepdims=True)
    twice = low * once_col + jnp.sum(m * inner_row, axis=1, keepdims=True)
    centre = jnp.sum(zt_ref[...] * twice, axis=0, keepdims=True) * inverse_norm

    scale = math.sqrt(diagonal) * jnp.sqrt(inverse_norm)
    m_parts = split(m * (scale * inverse_norm))
    small = eye(BLOCK)
    spot = lax.broadcasted_iota(jnp.int32, (16, BLOCK), 0)
    both = jnp.zeros((16, BLOCK), f32)
    at = 0
    for i in range(4):
        v = product(split(z_ref[i * BLOCK : (i + 1) * BLOCK, :]), m_parts)
        band = product(split(v), split(zt_ref[:, i * BLOCK :]))
        for j in range(i, 4):
            block = band[:, (j - i) * BLOCK : (j - i + 1) * BLOCK]
            if i == j:
                block = block + (scale * low) * small
            if i < 3:
                packed[at : at + BLOCK, :] = block.astype(bf16)
                at += BLOCK
                continue
            turned = pltpu.roll(block, 64, 1)
            quarters = (block[:64, :64], turned[:64, :64], turned[64:, :64])
            for d, quarter in enumerate(quarters):
                start = SPOTS[d, d] + 64
                packed[start : start + 64, :64] = quarter.astype(bf16)
        along = centre[:, i * BLOCK : (i + 1) * BLOCK]
        high = along.astype(bf16).astype(f32)
        both = both + jnp.where(spot == i, high, jnp.where(spot == 4 + i, along - high, 0.0))
    packed[CENTRE_AT:, :] = both.astype(bf16)


def region_weights(regions, tile, index, values, variances):
    return pl.pallas_call(
        weights_kernel,
        out_shape=jax.ShapeDtypeStruct((PACKED, BLOCK), bf16),
        in_specs=[vmem] * HALVES + [smem] + [vmem] * 3,
        out_specs=vmem,
        scratch_shapes=[
            pltpu.VMEM((MEMBERS, OBS), f32),
            pltpu.VMEM((OBS, MEMBERS), f32),
            pltpu.VMEM((OBS, OBS), f32),
            pltpu.VMEM((OBS, OBS), f32),
            pltpu.VMEM((OBS, OBS), f32),
            pltpu.VMEM((OBS, OBS), f32),
        ],
        compiler_params=pltpu.CompilerParams(vmem_limit_bytes=24 * 1024 * 1024),
        cost_estimate=pl.CostEstimate(flops=6_000_000_000, bytes_accessed=1_000_000, transcendentals=0),
        name="weights",
    )(
        *regions,
        tile,
        index,
        values,
        variances,
    )


def column_parts(columns, parity):
    place = lax.broadcasted_iota(jnp.int32, (1, columns), 1)
    row = 2 * (place // HALF) + (place // 64) % 2
    col = place % 64
    row_weight = jnp.abs((row.astype(f32) + 0.5) / 4.0 - 0.5)
    col_weight = jnp.abs((col.astype(f32) + 0.5) / 64.0 - 0.5)
    right = (col >= 32).astype(jnp.int32)
    sibling = ((right + parity) == 1).astype(f32)
    return row_weight, col_weight, sibling


def factors(parity):
    r, q, sibling = column_parts(COLS, parity)
    side = {0: 1.0 - q, 1: q * sibling, 2: q * (1.0 - sibling)}
    return {(row, s): (r if row else 1.0 - r) * side[s] for row in (0, 1) for s in (0, 1, 2)}


def unpack(source, full):
    row = lax.broadcasted_iota(jnp.int32, (BLOCK, BLOCK), 0)
    col = lax.broadcasted_iota(jnp.int32, (BLOCK, BLOCK), 1)
    free = (row >= 64) & (col < 64)

    def mirrored(block):
        return jnp.where(free, jnp.transpose(block), block).astype(bf16)

    for i, j in PAIRS[:-1]:
        block = source[SPOTS[i, j] : SPOTS[i, j] + BLOCK, :]
        if i == j:
            block = mirrored(block.astype(f32))
        else:
            full[j * BLOCK : (j + 1) * BLOCK, i * BLOCK : (i + 1) * BLOCK] = jnp.transpose(block)
        full[i * BLOCK : (i + 1) * BLOCK, j * BLOCK : (j + 1) * BLOCK] = block
    x, y, z = (
        source[SPOTS[d, d] + 64 : SPOTS[d, d] + BLOCK, :].astype(f32) for d in range(3)
    )
    top = jnp.where(col[:64] < 64, x, pltpu.roll(y, 64, 1))
    block = jnp.concatenate([top, pltpu.roll(z, 64, 1)], axis=0)
    full[3 * BLOCK : MEMBERS, 3 * BLOCK :] = mirrored(block)


def apply(source, full, dev, acc, lo, hi, factor, before=None, out=None):
    unpack(source, full)
    spot = lax.broadcasted_iota(jnp.int32, (16, BLOCK), 0)
    centre = source[CENTRE_AT:, :].astype(f32)
    for i in range(4):
        mine = jnp.where(spot % 4 == i, centre, 0.0)
        full[MEMBERS:, i * BLOCK : (i + 1) * BLOCK] = mine.astype(bf16)

    def part(at):
        both = dot(full[...], dev[:, at])
        shift = jnp.sum(both[MEMBERS:], axis=0, keepdims=True)
        term = factor[:, at] * (both[:MEMBERS] + shift)
        term = term + (acc[:, at] if before is None else before[:, at])
        if out is None:
            acc[:, at] = term
        else:
            out[:, :, at] = term.astype(bf16).reshape(out.shape[0], out.shape[1], HALF)

    for at in range(lo, hi, HALF):
        part(slice(at, at + HALF))


def own_kernel(*refs):
    parity = refs[0]
    regions = refs[1 : 1 + HALVES]
    own, acc, dev, full, mean_ref = refs[1 + HALVES :]
    size = MEMBERS // HALVES
    for g in range(COLS // BLOCK):
        at = slice(g * BLOCK, (g + 1) * BLOCK)
        parts = [part[:, at].astype(f32) for part in regions]
        mean = sum(jnp.sum(part, axis=0, keepdims=True) for part in parts) * (1.0 / MEMBERS)
        mean_ref[:, at] = mean
        for n, part in enumerate(parts):
            dev[n * size : (n + 1) * size, at] = (part - mean).astype(bf16)
    apply(own, full, dev, acc, 0, COLS, factors(parity[0])[0, 0], before=mean_ref)


def near_kernel(
    parity, acc_in, dev, sibling, other, below, above, acc, full
):
    factor = factors(parity[0])
    apply(sibling, full, dev, acc, 0, COLS, factor[0, 1])
    apply(other, full, dev, acc, 0, COLS, factor[0, 2])
    apply(below, full, dev, acc, 0, HALF, factor[1, 0])
    apply(above, full, dev, acc, HALF, COLS, factor[1, 0])


def side_kernel(parity, acc_in, dev, below_sibling, above_sibling, acc, full):
    factor = factors(parity[0])
    apply(below_sibling, full, dev, acc, 0, HALF, factor[1, 1])
    apply(above_sibling, full, dev, acc, HALF, COLS, factor[1, 1])


def far_kernel(
    parity, acc, dev, below_other, above_other, out, full
):
    factor = factors(parity[0])
    apply(below_other, full, dev, acc, 0, HALF, factor[1, 2], out=out)
    apply(above_other, full, dev, acc, HALF, COLS, factor[1, 2], out=out)


def call(kernel, outs, flops, scratch, parity, *arrays, alias=False):
    return pl.pallas_call(
    kernel,
    out_shape=outs,
    in_specs=[smem] + [vmem] * len(arrays),
    out_specs=jax.tree.map(lambda _: vmem, outs),
    scratch_shapes=[pltpu.VMEM((MEMBERS + 16, MEMBERS), bf16)] + scratch,
    input_output_aliases={1: 0} if alias else {},
    compiler_params=pltpu.CompilerParams(vmem_limit_bytes=16 * 1024 * 1024),
    cost_estimate=pl.CostEstimate(flops=flops, bytes_accessed=1_000_000, transcendentals=0),
    )(parity, *arrays)


def restore_kernel(back, out, held):
    low = lax.broadcasted_iota(jnp.int32, (GROUP, BLOCK), 1) < 64

    def group(g, carry):
        at = pl.ds(pl.multiple_of(g * GROUP, GROUP), GROUP)
        for f in range(3):
            for p in range(2):
                place = p * HALF + f * BLOCK
                for t in range(4):
                    x = back[2 * t, at, place : place + BLOCK].astype(f32)
                    y = back[2 * t + 1, at, place : place + BLOCK].astype(f32)
                    first = jnp.where(low, x, pltpu.roll(y, 64, 1))
                    second = jnp.where(low, pltpu.roll(x, 64, 1), y)
                    held[t, pl.ds(2 * p, GROUP, stride=4), :] = first
                    held[t, pl.ds(2 * p + 1, GROUP, stride=4), :] = second
            for t in range(4):
                rows = held[t, :, :].reshape(GROUP, 4, BLOCK)
                out[0, at, f, :, t * BLOCK : (t + 1) * BLOCK] = rows.astype(bf16)
        return carry

    lax.fori_loop(0, back.shape[1] // GROUP, group, 0)


def restored(back):
    tiles, members, _ = back.shape
    columns = tiles * 64
    return pl.pallas_call(
        restore_kernel,
        out_shape=jax.ShapeDtypeStruct((1, members, 3, 4, columns), bf16),
        in_specs=[vmem],
        out_specs=vmem,
        scratch_shapes=[pltpu.VMEM((4, GROUP * 4, BLOCK), f32)],
        compiler_params=pltpu.CompilerParams(vmem_limit_bytes=12 * 1024 * 1024),
        cost_estimate=pl.CostEstimate(flops=10_000_000, bytes_accessed=1_000_000, transcendentals=0),
        name="restore",
    )(back)


def program(ensemble, obs_index, obs_value, obs_var):
    bands = lax.axis_size("space")
    tiles = lax.axis_size("member")
    tile = lax.axis_index("member")
    up = [(i, (i + 1) % bands) for i in range(bands)]
    down = [(j, i) for i, j in up]
    sibling_pairs = [(i, i ^ 1) for i in range(tiles)]
    other_pairs = [(i, (i + 1) % tiles if i % 2 else (i - 1) % tiles) for i in range(tiles)]

    near_members = ensemble.shape[1]
    fields, tile = lax.optimization_barrier((ensemble[0].transpose(1, 2, 0, 3), tile))
    parity = (tile % 2).astype(jnp.int32).reshape(1)
    chunks = forecast(fields, up, down)
    region = lax.all_to_all(chunks, "member", 0, 0, tiled=True).reshape(MEMBERS, COLS)
    regions = [region]
    own = region_weights(regions, tile.reshape(1), obs_index[0, 0], obs_value[0, 0], obs_var[0, 0])

    other = lax.ppermute(own, "member", other_pairs)
    below = lax.ppermute(own, "space", up)
    above = lax.ppermute(own, "space", down)
    sibling = lax.ppermute(own, "member", sibling_pairs)
    below_other = lax.ppermute(other, "space", up)
    above_other = lax.ppermute(other, "space", down)
    below_sibling = lax.ppermute(below, "member", sibling_pairs)
    above_sibling = lax.ppermute(above, "member", sibling_pairs)
    total_shape = jax.ShapeDtypeStruct((MEMBERS, COLS), f32)
    dev_shape = jax.ShapeDtypeStruct((MEMBERS, COLS), bf16)
    out_shape = jax.ShapeDtypeStruct((tiles, near_members, COLS), bf16)
    mean_scratch = [pltpu.VMEM((1, COLS), f32)]
    acc, dev = call(own_kernel, (total_shape, dev_shape), 400_000_000, mean_scratch, parity, *regions, own)
    acc = call(near_kernel, total_shape, 1_200_000_000, [], parity, acc, dev, sibling, other, below, above, alias=True)
    acc = call(side_kernel, total_shape, 400_000_000, [], parity, acc, dev, below_sibling, above_sibling, alias=True)
    analysed = call(far_kernel, out_shape, 400_000_000, [], parity, acc, dev, below_other, above_other)
    back = lax.all_to_all(analysed, "member", 0, 0, tiled=True)
    return restored(back)


def solution(mesh):
    return jax.shard_map(
        program,
        mesh=mesh,
        in_specs=(
            P("group", "member", None, "space", None),
            P("group", "space", None, None),
            P("group", "space", "member", None),
            P("group", "space", "member", None),
        ),
        out_specs=P("group", "member", None, "space", None),
        check_vma=False,
    )
```

```python
import functools
import math

import jax
import jax.numpy as jnp
from jax import lax
from jax.experimental import pallas as pl
from jax.experimental.pallas import tpu as pltpu
from jax.sharding import PartitionSpec as P

NS_STEPS = 6
MEMBERS = 512
CELLS = 256
OBS = 256
BLOCK = 128
PAIRS = [(i, j) for i in range(4) for j in range(i, 4)]
SPOTS = {pair: n * BLOCK for n, pair in enumerate(PAIRS)}
CENTRE_AT = SPOTS[3, 3]
PACKED = CENTRE_AT + 16

time_step = 0.4
coriolis = 0.3
COLS = 768
HALF = 384
HALVES = 1
PARTS = 2
f32 = jnp.float32
bf16 = jnp.bfloat16
vmem = pl.BlockSpec(memory_space=pltpu.VMEM)
smem = pl.BlockSpec(memory_space=pltpu.SMEM)


def column_difference(field):
    columns = field.shape[-1]
    return 0.5 * (pltpu.roll(field, columns - 1, 1) - pltpu.roll(field, 1, 1))


def rates(h, v, u, i):
    d_height = -(column_difference(u[i]) + 0.5 * (v[i + 1] - v[i - 1]))
    d_north = -0.5 * (h[i + 1] - h[i - 1]) - coriolis * u[i]
    return d_height, d_north


def rate_east(h, v, i):
    return coriolis * v[i] - column_difference(h[i])


def advance(h0, v0, u0):
    h1, v1, u1, h2, v2, u2, h3, v3, u3 = ({} for _ in range(9))
    for i in range(-2, 6):
        dh, dv = rates(h0, v0, u0, i)
        h1[i] = h0[i] + time_step * dh
        v1[i] = v0[i] + time_step * dv
        if -1 <= i <= 4:
            u1[i] = u0[i] + time_step * rate_east(h0, v0, i)
    for i in range(-1, 5):
        dh, dv = rates(h1, v1, u1, i)
        h2[i] = 0.75 * h0[i] + 0.25 * (h1[i] + time_step * dh)
        v2[i] = 0.75 * v0[i] + 0.25 * (v1[i] + time_step * dv)
        if 0 <= i <= 3:
            u2[i] = 0.75 * u0[i] + 0.25 * (u1[i] + time_step * rate_east(h1, v1, i))
    third = 1.0 / 3.0
    two_thirds = 2.0 / 3.0
    for i in range(4):
        dh, dv = rates(h2, v2, u2, i)
        h3[i] = h0[i] * third + two_thirds * (h2[i] + time_step * dh)
        v3[i] = v0[i] * third + two_thirds * (v2[i] + time_step * dv)
        u3[i] = u0[i] * third + two_thirds * (u2[i] + time_step * rate_east(h2, v2, i))
    return h3, v3, u3


GROUP = 16


def loaded(now, below, above, at):
    h, v, u = {}, {}, {}
    for f, field in enumerate((h, v, u)):
        for i in range(4):
            field[i] = now[f, i, at, :].astype(f32)
    for k in range(3):
        h[k - 3] = below[k, at, :].astype(f32)
        v[k - 3] = below[3 + k, at, :].astype(f32)
        h[4 + k] = above[k, at, :].astype(f32)
        v[4 + k] = above[3 + k, at, :].astype(f32)
    for k in range(2):
        u[k - 2] = below[6 + k, at, :].astype(f32)
        u[4 + k] = above[6 + k, at, :].astype(f32)
    return h, v, u


def first_step_kernel(now, below, above, out, first, last):
    def group(g, carry):
        at = pl.ds(pl.multiple_of(g * GROUP, GROUP), GROUP)
        fields = advance(*loaded(now, below, above, at))
        for f in range(3):
            edge = 2 if f == 2 else 3
            for i in range(4):
                out[f, i, at, :] = fields[f][i]
                if i < edge:
                    first[3 * f + i, at, :] = fields[f][i].astype(bf16)
                if i >= 4 - edge:
                    last[3 * f + i - (4 - edge), at, :] = fields[f][i].astype(bf16)
        return carry

    lax.fori_loop(0, now.shape[2] // GROUP, group, 0)


def last_step_kernel(base, now, below, above, *refs):
    out = refs[-1]
    lane = lax.broadcasted_iota(jnp.int32, (GROUP, BLOCK), 1) < 64

    def group(g, carry):
        at = pl.ds(pl.multiple_of(g * GROUP, GROUP), GROUP)
        into = pl.ds(pl.multiple_of(base + g * GROUP, GROUP), GROUP)
        fields = advance(*loaded(now, below, above, at))
        for f in range(3):
            for p in range(2):
                to = p * HALF + f * BLOCK
                for t in range(4):
                    x = fields[f][2 * p][:, t * BLOCK : (t + 1) * BLOCK]
                    y = fields[f][2 * p + 1][:, t * BLOCK : (t + 1) * BLOCK]
                    even = jnp.where(lane, x, pltpu.roll(y, 64, 1))
                    odd = jnp.where(lane, pltpu.roll(x, 64, 1), y)
                    out[2 * t, into, to : to + BLOCK] = even.astype(bf16)
                    out[2 * t + 1, into, to : to + BLOCK] = odd.astype(bf16)
        return carry

    lax.fori_loop(0, now.shape[2] // GROUP, group, 0)


def swapped(last, first, up, down):
    return lax.ppermute(last, "space", up), lax.ppermute(first, "space", down)


def edges(fields):
    last = jnp.concatenate([fields[0, 1:], fields[1, 1:], fields[2, 2:]], axis=0)
    first = jnp.concatenate([fields[0, :3], fields[1, :3], fields[2, :2]], axis=0)
    return last, first


def step(kernel, outs, *arrays, aliases={}):
    return pl.pallas_call(
        kernel,
        out_shape=outs,
        in_specs=[vmem] * len(arrays),
        out_specs=jax.tree.map(lambda _: vmem, outs),
        input_output_aliases=aliases,
        compiler_params=pltpu.CompilerParams(vmem_limit_bytes=12 * 1024 * 1024),
        cost_estimate=pl.CostEstimate(
            flops=100_000_000 // PARTS, bytes_accessed=1_000_000, transcendentals=0
        ),
    )(*arrays)


def forecast(fields, up, down):
    _, rows, members, columns = fields.shape
    half = members // PARTS
    now_shape = jax.ShapeDtypeStruct((3, rows, half, columns), f32)
    edge_shape = jax.ShapeDtypeStruct((8, half, columns), bf16)
    chunk_shape = jax.ShapeDtypeStruct((columns // 64, members, COLS), bf16)
    parts = [fields[:, :, n * half : (n + 1) * half] for n in range(PARTS)]
    halos = [swapped(*edges(part), up, down) for part in parts]
    first_outs = (now_shape, edge_shape, edge_shape)
    chunks = ()
    for n in range(PARTS):
        now, first, last = step(first_step_kernel, first_outs, parts[n], *halos[n])
        halo = swapped(last, first, up, down)
        kernel = functools.partial(last_step_kernel, n * half)
        aliases = {3: 0} if chunks else {}
        chunks = (step(kernel, chunk_shape, now, *halo, *chunks, aliases=aliases),)
    return chunks[0]


def dot(a, b):
    return jnp.dot(a, b, preferred_element_type=f32)


def dot_t(a, b):
    return lax.dot_general(a, b, (((1,), (1,)), ((), ())), preferred_element_type=f32)


def split(a):
    high = a.astype(bf16)
    return high, (a - high.astype(f32)).astype(bf16)


def product(a, b):
    return dot(a[0], b[0]) + (dot(a[0], b[1]) + dot(a[1], b[0]))


def eye(n):
    return (
        lax.broadcasted_iota(jnp.int32, (n, n), 0) == lax.broadcasted_iota(jnp.int32, (n, n), 1)
    ).astype(f32)


def total(a):
    return jnp.sum(jnp.sum(a, axis=1, keepdims=True), axis=0, keepdims=True)


def weights_kernel(*refs):
    regions = refs[:HALVES]
    tile, index, value, var, packed = refs[HALVES : HALVES + 5]
    z_ref, zt_ref, b_ref, m_ref, l_ref, u_ref = refs[HALVES + 5 :]
    identity = eye(OBS)

    def as_column(row):
        return jnp.sum(identity * row, axis=1, keepdims=True)

    index_row = index[pl.ds(tile[0], 1), :]
    index_col = as_column(index_row.astype(f32)).astype(jnp.int32)
    var_row = var[...]
    var_col = as_column(var_row)
    own = jnp.concatenate(
        [
            jnp.concatenate([part[:, :BLOCK], part[:, HALF : HALF + BLOCK]], axis=1)
            for part in regions
        ],
        axis=0,
    )
    cell_row = lax.broadcasted_iota(jnp.int32, (CELLS, OBS), 0)
    pick = (cell_row == index_row).astype(f32).astype(bf16)
    cell_col = lax.broadcasted_iota(jnp.int32, (OBS, CELLS), 1)
    pick_t = (cell_col == index_col).astype(f32).astype(bf16)
    y = dot(own, pick)
    mean_row = jnp.sum(y, axis=0, keepdims=True) * (1.0 / MEMBERS)
    inverse_row = lax.rsqrt(var_row)
    z_ref[...] = (y - mean_row) * inverse_row
    y_t = dot_t(pick_t, own)
    mean_col = jnp.sum(y_t, axis=1, keepdims=True) * (1.0 / MEMBERS)
    zt_ref[...] = (y_t - mean_col) * lax.rsqrt(var_col)
    w_row = (value[...] - mean_row) * inverse_row

    b = product(split(zt_ref[...]), split(z_ref[...]))
    diagonal = float(MEMBERS - 1)
    squared = diagonal * diagonal * MEMBERS + 2.0 * diagonal * total(b * identity) + total(b * b)
    inverse_norm = lax.rsqrt(squared)
    alpha = diagonal * inverse_norm
    b = b * inverse_norm
    b_ref[...] = b

    low = 1.5 - 0.5 * alpha
    lower = low * identity - 0.5 * b
    l_ref[...] = lower
    u_ref[...] = alpha * lower + product(split(b), split(lower))
    m_ref[...] = -0.5 * identity

    def one_step(_, low):
        identity = eye(OBS)
        m = m_ref[...]
        lower = l_ref[...]
        l_parts = split(lower)
        u_parts = split(u_ref[...])
        step = split(1.5 * identity - 0.5 * product(l_parts, u_parts))
        part = split(-0.5 * (low * (alpha * m + lower) + product(split(m), u_parts)))
        factor = 1.5 - 0.5 * alpha * low * low
        l_ref[...] = product(step, l_parts)
        m_ref[...] = factor * m + product(part, l_parts)
        u_ref[...] = product(step, u_parts)
        return factor * low

    low = lax.fori_loop(0, NS_STEPS - 2, one_step, low)
    m = m_ref[...]
    lower = l_ref[...]
    part = -0.5 * (low * (alpha * m + lower) + product(split(m), split(u_ref[...])))
    factor = 1.5 - 0.5 * alpha * low * low
    m = factor * m + product(split(part), split(lower))
    low = factor * low

    b = b_ref[...]
    once = low * w_row + jnp.sum(
        m * jnp.sum(b * w_row, axis=1, keepdims=True), axis=0, keepdims=True
    )
    inner = jnp.sum(b * once, axis=1, keepdims=True)
    once_col = jnp.sum(identity * once, axis=1, keepdims=True)
    inner_row = jnp.sum(identity * inner, axis=0, keepdims=True)
    twice = low * once_col + jnp.sum(m * inner_row, axis=1, keepdims=True)
    centre = jnp.sum(zt_ref[...] * twice, axis=0, keepdims=True) * inverse_norm

    scale = math.sqrt(diagonal) * jnp.sqrt(inverse_norm)
    m_parts = split(m * (scale * inverse_norm))
    small = eye(BLOCK)
    spot = lax.broadcasted_iota(jnp.int32, (16, BLOCK), 0)
    both = jnp.zeros((16, BLOCK), f32)
    at = 0
    v_high, v_low = split(product(split(z_ref[...]), m_parts))
    zt_high, zt_low = split(zt_ref[...])
    for i in range(4):
        rows = slice(i * BLOCK, (i + 1) * BLOCK)
        right = (zt_high[:, i * BLOCK :], zt_low[:, i * BLOCK :])
        band = product((v_high[rows], v_low[rows]), right)
        for j in range(i, 4):
            block = band[:, (j - i) * BLOCK : (j - i + 1) * BLOCK]
            if i == j:
                block = block + (scale * low) * small
            if i < 3:
                packed[at : at + BLOCK, :] = block.astype(bf16)
                at += BLOCK
                continue
            turned = pltpu.roll(block, 64, 1)
            quarters = (block[:64, :64], turned[:64, :64], turned[64:, :64])
            for d, quarter in enumerate(quarters):
                start = SPOTS[d, d] + 64
                packed[start : start + 64, :64] = quarter.astype(bf16)
        along = centre[:, i * BLOCK : (i + 1) * BLOCK]
        high = along.astype(bf16).astype(f32)
        both = both + jnp.where(spot == i, high, jnp.where(spot == 4 + i, along - high, 0.0))
    packed[CENTRE_AT:, :] = both.astype(bf16)


def region_weights(regions, tile, index, values, variances):
    return pl.pallas_call(
        weights_kernel,
        out_shape=jax.ShapeDtypeStruct((PACKED, BLOCK), bf16),
        in_specs=[vmem] * HALVES + [smem] + [vmem] * 3,
        out_specs=vmem,
        scratch_shapes=[
            pltpu.VMEM((MEMBERS, OBS), f32),
            pltpu.VMEM((OBS, MEMBERS), f32),
            pltpu.VMEM((OBS, OBS), f32),
            pltpu.VMEM((OBS, OBS), f32),
            pltpu.VMEM((OBS, OBS), f32),
            pltpu.VMEM((OBS, OBS), f32),
        ],
        compiler_params=pltpu.CompilerParams(vmem_limit_bytes=24 * 1024 * 1024),
        cost_estimate=pl.CostEstimate(flops=6_000_000_000, bytes_accessed=1_000_000, transcendentals=0),
        name="weights",
    )(
        *regions,
        tile,
        index,
        values,
        variances,
    )


def column_parts(columns, parity):
    place = lax.broadcasted_iota(jnp.int32, (1, columns), 1)
    row = 2 * (place // HALF) + (place // 64) % 2
    col = place % 64
    row_weight = jnp.abs((row.astype(f32) + 0.5) / 4.0 - 0.5)
    col_weight = jnp.abs((col.astype(f32) + 0.5) / 64.0 - 0.5)
    right = (col >= 32).astype(jnp.int32)
    sibling = ((right + parity) == 1).astype(f32)
    return row_weight, col_weight, sibling


def factors(parity):
    r, q, sibling = column_parts(COLS, parity)
    side = {0: 1.0 - q, 1: q * sibling, 2: q * (1.0 - sibling)}
    return {(row, s): (r if row else 1.0 - r) * side[s] for row in (0, 1) for s in (0, 1, 2)}


def unpack(source, full):
    row = lax.broadcasted_iota(jnp.int32, (BLOCK, BLOCK), 0)
    col = lax.broadcasted_iota(jnp.int32, (BLOCK, BLOCK), 1)
    free = (row >= 64) & (col < 64)

    def mirrored(block):
        return jnp.where(free, jnp.transpose(block), block).astype(bf16)

    for i, j in PAIRS[:-1]:
        block = source[SPOTS[i, j] : SPOTS[i, j] + BLOCK, :]
        if i == j:
            block = mirrored(block.astype(f32))
        else:
            full[j * BLOCK : (j + 1) * BLOCK, i * BLOCK : (i + 1) * BLOCK] = jnp.transpose(block)
        full[i * BLOCK : (i + 1) * BLOCK, j * BLOCK : (j + 1) * BLOCK] = block
    x, y, z = (
        source[SPOTS[d, d] + 64 : SPOTS[d, d] + BLOCK, :].astype(f32) for d in range(3)
    )
    top = jnp.where(col[:64] < 64, x, pltpu.roll(y, 64, 1))
    block = jnp.concatenate([top, pltpu.roll(z, 64, 1)], axis=0)
    full[3 * BLOCK : MEMBERS, 3 * BLOCK :] = mirrored(block)


def apply(source, full, dev, acc, lo, hi, factor, before=None, out=None):
    unpack(source, full)
    spot = lax.broadcasted_iota(jnp.int32, (16, BLOCK), 0)
    centre = source[CENTRE_AT:, :].astype(f32)
    for i in range(4):
        mine = jnp.where(spot % 4 == i, centre, 0.0)
        full[MEMBERS:, i * BLOCK : (i + 1) * BLOCK] = mine.astype(bf16)

    def part(at):
        both = dot(full[...], dev[:, at])
        shift = jnp.sum(both[MEMBERS:], axis=0, keepdims=True)
        term = factor[:, at] * (both[:MEMBERS] + shift)
        term = term + (acc[:, at] if before is None else before[:, at])
        if out is None:
            acc[:, at] = term
        else:
            out[:, :, at] = term.astype(bf16).reshape(out.shape[0], out.shape[1], HALF)

    for at in range(lo, hi, HALF):
        part(slice(at, at + HALF))


def own_kernel(*refs):
    parity = refs[0]
    regions = refs[1 : 1 + HALVES]
    own, acc, dev, full, mean_ref = refs[1 + HALVES :]
    size = MEMBERS // HALVES
    for g in range(COLS // BLOCK):
        at = slice(g * BLOCK, (g + 1) * BLOCK)
        parts = [part[:, at].astype(f32) for part in regions]
        mean = sum(jnp.sum(part, axis=0, keepdims=True) for part in parts) * (1.0 / MEMBERS)
        mean_ref[:, at] = mean
        for n, part in enumerate(parts):
            dev[n * size : (n + 1) * size, at] = (part - mean).astype(bf16)
    apply(own, full, dev, acc, 0, COLS, factors(parity[0])[0, 0], before=mean_ref)


def near_kernel(
    parity, acc_in, dev, sibling, other, below, above, acc, full
):
    factor = factors(parity[0])
    apply(sibling, full, dev, acc, 0, COLS, factor[0, 1])
    apply(other, full, dev, acc, 0, COLS, factor[0, 2])
    apply(below, full, dev, acc, 0, HALF, factor[1, 0])
    apply(above, full, dev, acc, HALF, COLS, factor[1, 0])


def side_kernel(parity, acc_in, dev, below_sibling, above_sibling, acc, full):
    factor = factors(parity[0])
    apply(below_sibling, full, dev, acc, 0, HALF, factor[1, 1])
    apply(above_sibling, full, dev, acc, HALF, COLS, factor[1, 1])


def far_kernel(
    parity, acc, dev, below_other, above_other, out, full
):
    factor = factors(parity[0])
    apply(below_other, full, dev, acc, 0, HALF, factor[1, 2], out=out)
    apply(above_other, full, dev, acc, HALF, COLS, factor[1, 2], out=out)


def call(kernel, outs, flops, scratch, parity, *arrays, alias=False):
    return pl.pallas_call(
    kernel,
    out_shape=outs,
    in_specs=[smem] + [vmem] * len(arrays),
    out_specs=jax.tree.map(lambda _: vmem, outs),
    scratch_shapes=[pltpu.VMEM((MEMBERS + 16, MEMBERS), bf16)] + scratch,
    input_output_aliases={1: 0} if alias else {},
    compiler_params=pltpu.CompilerParams(vmem_limit_bytes=16 * 1024 * 1024),
    cost_estimate=pl.CostEstimate(flops=flops, bytes_accessed=1_000_000, transcendentals=0),
    )(parity, *arrays)


def restore_kernel(back, out, held):
    low = lax.broadcasted_iota(jnp.int32, (GROUP, BLOCK), 1) < 64

    def group(g, carry):
        at = pl.ds(pl.multiple_of(g * GROUP, GROUP), GROUP)
        for f in range(3):
            for p in range(2):
                place = p * HALF + f * BLOCK
                for t in range(4):
                    x = back[2 * t, at, place : place + BLOCK].astype(f32)
                    y = back[2 * t + 1, at, place : place + BLOCK].astype(f32)
                    first = jnp.where(low, x, pltpu.roll(y, 64, 1))
                    second = jnp.where(low, pltpu.roll(x, 64, 1), y)
                    held[t, pl.ds(2 * p, GROUP, stride=4), :] = first
                    held[t, pl.ds(2 * p + 1, GROUP, stride=4), :] = second
            for t in range(4):
                rows = held[t, :, :].reshape(GROUP, 4, BLOCK)
                out[0, at, f, :, t * BLOCK : (t + 1) * BLOCK] = rows.astype(bf16)
        return carry

    lax.fori_loop(0, back.shape[1] // GROUP, group, 0)


def restored(back):
    tiles, members, _ = back.shape
    columns = tiles * 64
    return pl.pallas_call(
        restore_kernel,
        out_shape=jax.ShapeDtypeStruct((1, members, 3, 4, columns), bf16),
        in_specs=[vmem],
        out_specs=vmem,
        scratch_shapes=[pltpu.VMEM((4, GROUP * 4, BLOCK), f32)],
        compiler_params=pltpu.CompilerParams(vmem_limit_bytes=12 * 1024 * 1024),
        cost_estimate=pl.CostEstimate(flops=10_000_000, bytes_accessed=1_000_000, transcendentals=0),
        name="restore",
    )(back)


def program(ensemble, obs_index, obs_value, obs_var):
    bands = lax.axis_size("space")
    tiles = lax.axis_size("member")
    tile = lax.axis_index("member")
    up = [(i, (i + 1) % bands) for i in range(bands)]
    down = [(j, i) for i, j in up]
    sibling_pairs = [(i, i ^ 1) for i in range(tiles)]
    other_pairs = [(i, (i + 1) % tiles if i % 2 else (i - 1) % tiles) for i in range(tiles)]

    near_members = ensemble.shape[1]
    fields, tile = lax.optimization_barrier((ensemble[0].transpose(1, 2, 0, 3), tile))
    parity = (tile % 2).astype(jnp.int32).reshape(1)
    chunks = forecast(fields, up, down)
    region = lax.all_to_all(chunks, "member", 0, 0, tiled=True).reshape(MEMBERS, COLS)
    regions = [region]
    own = region_weights(regions, tile.reshape(1), obs_index[0, 0], obs_value[0, 0], obs_var[0, 0])

    other = lax.ppermute(own, "member", other_pairs)
    below = lax.ppermute(own, "space", up)
    above = lax.ppermute(own, "space", down)
    sibling = lax.ppermute(own, "member", sibling_pairs)
    below_other = lax.ppermute(other, "space", up)
    above_other = lax.ppermute(other, "space", down)
    below_sibling = lax.ppermute(below, "member", sibling_pairs)
    above_sibling = lax.ppermute(above, "member", sibling_pairs)
    total_shape = jax.ShapeDtypeStruct((MEMBERS, COLS), f32)
    dev_shape = jax.ShapeDtypeStruct((MEMBERS, COLS), bf16)
    out_shape = jax.ShapeDtypeStruct((tiles, near_members, COLS), bf16)
    mean_scratch = [pltpu.VMEM((1, COLS), f32)]
    acc, dev = call(own_kernel, (total_shape, dev_shape), 400_000_000, mean_scratch, parity, *regions, own)
    acc = call(near_kernel, total_shape, 1_200_000_000, [], parity, acc, dev, sibling, other, below, above, alias=True)
    acc = call(side_kernel, total_shape, 400_000_000, [], parity, acc, dev, below_sibling, above_sibling, alias=True)
    analysed = call(far_kernel, out_shape, 400_000_000, [], parity, acc, dev, below_other, above_other)
    back = lax.all_to_all(analysed, "member", 0, 0, tiled=True)
    return restored(back)


def solution(mesh):
    return jax.shard_map(
        program,
        mesh=mesh,
        in_specs=(
            P("group", "member", None, "space", None),
            P("group", "space", None, None),
            P("group", "space", "member", None),
            P("group", "space", "member", None),
        ),
        out_specs=P("group", "member", None, "space", None),
        check_vma=False,
    )
```
